128 devices in a mesh: section: 8 (over x_hi, z), fsdp: 16 (over y, x_lo, core).
Axes of the slice: x: 4 (x_hi: 2, x_lo: 2; x = x_hi * 2 + x_lo), y: 4, z: 4, core: 2. Of those that a mesh axis runs over, the one named last changes fastest.
Arguments:
- hidden_in: bfloat16 [8, 16, 64, 1536], P(None, 'fsdp'), may hold values from -6 to 6
- norm_gain: float32 [2, 8, 1536], P(None, 'section'), may hold values from 0.25 to 1.75
- qkv_weight: bfloat16 [2, 8, 1536, 2048], P(None, 'section', 'fsdp'), may hold values from -0.15625 to 0.15625
- qkv_bias: float32 [2, 8, 2048], P(None, 'section'), may hold values from -30 to 30, as said below
- out_weight: bfloat16 [2, 8, 1536, 1536], P(None, 'section', 'fsdp'), may hold values from -0.15625 to 0.15625
Outputs:
- hidden_out: bfloat16 [8, 16, 64, 1536], P('section', 'fsdp')
The draws below stay inside these ranges and needn't reach their ends.
Inputs may be any that keep to these rules, and one draw needn't show every extreme that they name: `qkv_bias`: entries of the query, key and value biases.
All inputs are finite; a program needn't handle non-finite values.
Results may differ from the reference program's by a relative error of at most 0.035.
Values may be sent and summed in bfloat16 or wider, within the bound.
A program may use at most 128 MiB of HBM per device.

```python
import math
import jax
import jax.numpy as jnp
from jax import lax

D = 1536
HEADS = 12
KV_HEADS = 2
HEAD_DIM = 128
LEN = 64
MICRO = 8
SPANS = 2
SEQS = 16
QKV = 2048
N_SECTION = 8


def draw_qkv_bias(key, part):
    bias_shape = (SPANS, N_SECTION, QKV)
    return jnp.clip(0.5 * jax.random.normal(key, bias_shape, jnp.float32), -3.0, 3.0)


def block_levels(key, extent, shards, least, top_value):
    def one(position, shards_of):
        heights = jax.random.uniform(jax.random.fold_in(jax.random.fold_in(key, 6), position), (shards_of,), jnp.float32, least / len(shards), top_value / len(shards))
        return jnp.repeat(jnp.exp(heights), extent[position] // shards_of).reshape((-1,) + (1,) * (len(extent) - position - 1))

    loudness = one(*shards[0])
    for cut in shards[1:]:
        loudness = loudness * one(*cut)
    return loudness


def scatter_about(stream_key, dims, deviation, most, split=(), kind=jnp.bfloat16):
    values = jax.random.normal(stream_key, dims, jnp.float32) * deviation
    if len(split) > 0:
        values = block_levels(stream_key, dims, split, -0.22, 0.18) * values
    return jnp.clip(values, min=-most, max=most).astype(kind)


def setup_inputs(seed: int = 0) -> dict:
    arg_keys = jax.random.split(jax.random.key(seed), 6)
    return {
        "hidden_in": scatter_about(arg_keys[0], (MICRO, SEQS, LEN, D), 1.0, 6.0, ((1, 16),)),
        "norm_gain": jnp.clip(1.0 + 0.15 * jax.random.normal(arg_keys[1], (SPANS, N_SECTION, D), jnp.float32), 0.25, 1.75),
        "qkv_weight": scatter_about(arg_keys[2], (SPANS, N_SECTION, D, QKV), D ** -0.5, 0.15625, ((1, 8), (2, 16))),
        "qkv_bias": draw_qkv_bias(jax.random.fold_in(arg_keys[5], 71), 0),
        "out_weight": scatter_about(arg_keys[4], (SPANS, N_SECTION, D, D), D ** -0.5, 0.15625, ((1, 8), (2, 16))),
    }


THETA = 1000000.0
EPS = 1.0

def rotate(tensor, cosine, sine_part):
    half_dim = tensor.shape[-1] // 2
    leading = tensor[..., :half_dim]
    second = tensor[..., half_dim:]
    return jnp.concatenate([leading * cosine - second * sine_part, second * cosine + leading * sine_part], axis=-1)

def attend_layer(hidden, gain, w_qkv, bias, w_out):
    rows, length, width = hidden.shape
    group_size = HEADS // KV_HEADS
    kv_width = KV_HEADS * HEAD_DIM
    wide = hidden.astype(jnp.float32)
    inv_rms = lax.rsqrt(lax.optimization_barrier(jnp.mean(wide * wide, axis=-1, keepdims=True)) + EPS)
    normed = (wide * inv_rms * gain).astype(jnp.bfloat16)
    projected = jnp.dot(normed.reshape(rows * length, width), w_qkv, preferred_element_type=jnp.float32) + bias
    projected = projected.reshape(rows, length, width + 2 * kv_width)
    queries = projected[..., :width].reshape(rows, length, KV_HEADS, group_size, HEAD_DIM)
    key_rows = projected[..., width:width + kv_width].reshape(rows, length, KV_HEADS, HEAD_DIM)
    value_rows = projected[..., width + kv_width:].astype(jnp.bfloat16).reshape(rows, length, KV_HEADS, HEAD_DIM)
    half_dim = HEAD_DIM // 2
    frequency = jnp.exp(jnp.arange(half_dim, dtype=jnp.float32) * (-2.0 * math.log(THETA) / HEAD_DIM))
    angles = jnp.arange(length, dtype=jnp.float32)[:, None] * frequency[None, :]
    cosine = jnp.cos(angles)
    sine_part = jnp.sin(angles)
    queries = rotate(queries, cosine[None, :, None, None, :], sine_part[None, :, None, None, :])
    key_rows = rotate(key_rows, cosine[None, :, None, :], sine_part[None, :, None, :])
    scores = jnp.einsum('rqkgd,rpkd->rkgqp', queries, key_rows, precision=lax.Precision.HIGHEST) / math.sqrt(HEAD_DIM)
    causal = jnp.arange(length)[:, None] >= jnp.arange(length)[None, :]
    scores = jnp.where(causal, scores, -1e+30)
    row_max = lax.optimization_barrier(jnp.max(scores, axis=-1, keepdims=True))
    weights = jnp.exp(scores - row_max)
    probability = (weights / lax.optimization_barrier(jnp.sum(weights, axis=-1, keepdims=True))).astype(jnp.bfloat16)
    context = jnp.einsum('rkgqp,rpkd->rqkgd', probability.astype(jnp.float32), value_rows.astype(jnp.float32), precision=lax.Precision.HIGHEST)
    context = context.reshape(rows, length, width).astype(jnp.bfloat16)
    update = jnp.dot(context.reshape(rows * length, width), w_out, preferred_element_type=jnp.float32)
    return (wide + update.reshape(rows, length, width)).astype(jnp.bfloat16)

def reference(hidden_in, norm_gain, qkv_weight, qkv_bias, out_weight):
    hidden = hidden_in
    for span_no in range(norm_gain.shape[0]):
        for section_no in range(norm_gain.shape[1]):

            def apply_layer(block_rows, span_no=span_no, section_no=section_no):
                return attend_layer(block_rows, norm_gain[span_no, section_no], qkv_weight[span_no, section_no], qkv_bias[span_no, section_no], out_weight[span_no, section_no])
            hidden = lax.map(apply_layer, hidden)
    return hidden
```

```python
import functools
import math

import jax
import jax.numpy as jnp
import numpy as np
from jax import lax
from jax.experimental import pallas as pl
from jax.experimental.pallas import tpu as pltpu
from jax.sharding import PartitionSpec as P

HEADS = 12
KV_HEADS = 2
HEAD_DIM = 128
GROUP = HEADS // KV_HEADS
LEN = 64
D = HEADS * HEAD_DIM
QKV = D + 2 * KV_HEADS * HEAD_DIM
SECTIONS = 8
FSDP = 16
ROWS = D // FSDP
HALF = ROWS // 2
MICRO = 8
STEPS = 2 * MICRO
CHUNKS = 3
CW = D // CHUNKS
FINAL = STEPS
THETA = 1000000.0
EPS = 1.0
EVENTS = 16
MESH = pl.DeviceIdType.MESH


def tables():
    frequency = np.exp(np.arange(HEAD_DIM // 2) * (-2.0 * math.log(THETA) / HEAD_DIM))
    angles = np.arange(LEN)[:, None] * frequency[None, :]
    cosine, sine = np.cos(angles), np.sin(angles)
    full_cos = np.concatenate([cosine, cosine], axis=1)
    full_sin = np.concatenate([-sine, sine], axis=1)
    scale = 1.0 / math.sqrt(HEAD_DIM)
    mask = np.where(np.arange(LEN)[:, None] >= np.arange(LEN)[None, :], 0.0, -1e30)
    rope = np.stack([full_cos * scale, full_sin * scale, full_cos, full_sin])
    return rope.astype(np.float32), mask.astype(np.float32)


def split_two(value):
    high = value.astype(jnp.bfloat16)
    low = (value - high.astype(jnp.float32)).astype(jnp.bfloat16)
    return high, low


def kernel(
    hidden_hbm,
    gain_ref,
    qkv_hbm,
    bias_ref,
    out_hbm,
    rope_ref,
    mask_ref,
    result_ref,
    wq,
    wo,
    inbox,
    outbox,
    acc,
    ctx,
    own_sem,
    gsend,
    grecv,
    hsend,
    hrecv,
):
    s = lax.axis_index("section")
    f = lax.axis_index("fsdp")
    y = lax.div(f, 4)
    low = lax.rem(f, 4)
    x = lax.div(low, 2)
    core = lax.rem(f, 2)
    mirrored = f + 2 - 4 * x
    x_other = low + 2 - 4 * x
    y_next = lax.rem(y + 1, 4) * 4
    y_prev = lax.rem(y + 3, 4) * 4
    y_far = lax.rem(y + 2, 4) * 4
    flip = 1 - 2 * core

    dev_next = y_next + low
    dev_prev = y_prev + low
    dev_x = mirrored
    dev_sib = f + flip

    blocks = (
        f,
        y_prev + low,
        y_next + low,
        mirrored,
        y_far + low,
        y_prev + x_other,
        y_next + x_other,
        y_far + x_other,
    )
    OWN, PREV, NEXT, ACROSS, FAR, XPREV, XNEXT, XFAR = blocks

    tensors = ((wq, 0), (wo, 0), (wq, 1), (wo, 1))
    sources = ((qkv_hbm, 0), (out_hbm, 0), (qkv_hbm, 1), (out_hbm, 1))

    def region(t, block, first=0, count=ROWS):
        ref, layer = tensors[t]
        start = pl.multiple_of(block * ROWS + first, 16)
        return ref.at[layer, pl.ds(start, count), :]

    sends = {
        0: (OWN, 0, ROWS, dev_next),
        1: (OWN, 0, ROWS, dev_prev),
        2: (OWN, 0, ROWS, dev_x),
        3: (PREV, 0, HALF, dev_next),
        4: (NEXT, HALF, HALF, dev_prev),
        5: (ACROSS, 0, ROWS, dev_next),
        6: (ACROSS, 0, ROWS, dev_prev),
        7: (FAR, 0, ROWS, dev_x),
    }
    lands = {
        0: (PREV, 0, ROWS),
        1: (NEXT, 0, ROWS),
        2: (ACROSS, 0, ROWS),
        3: (FAR, 0, HALF),
        4: (FAR, HALF, HALF),
        5: (XPREV, 0, ROWS),
        6: (XNEXT, 0, ROWS),
        7: (XFAR, 0, ROWS),
    }
    for n in range(8):
        sends[8 + n] = (blocks[n], 0, ROWS, dev_sib)
        lands[8 + n] = (blocks[n] + flip, 0, ROWS)

    def outgoing(t, e):
        block, first, count, target = sends[e]
        part = region(t, block, first, count)
        return pltpu.make_async_remote_copy(
            src_ref=part,
            dst_ref=part,
            send_sem=gsend.at[t, e],
            recv_sem=grecv.at[t, e],
            device_id=(s, target),
            device_id_type=MESH,
        )

    def arrived(t, e):
        block, first, count = lands[e]
        part = region(t, block, first, count)
        pltpu.make_async_remote_copy(
            src_ref=part,
            dst_ref=part,
            send_sem=gsend.at[t, e],
            recv_sem=grecv.at[t, e],
            device_id=(s, dev_sib),
            device_id_type=MESH,
        ).wait_recv()

    def own_copy(t):
        ref, layer = sources[t]
        return pltpu.make_async_copy(ref.at[layer, 0], region(t, OWN), own_sem.at[t])

    def gather_a(t):
        own_copy(t).wait()
        for e in (0, 1, 2, 8):
            outgoing(t, e).start()

    def gather_b(t):
        for e, then in ((0, (3, 9)), (1, (4, 10)), (2, (5, 6, 11))):
            arrived(t, e)
            for n in then:
                outgoing(t, n).start()

    def gather_c(t):
        arrived(t, 3)
        arrived(t, 4)
        for n in (7, 12):
            outgoing(t, n).start()
        arrived(t, 5)
        outgoing(t, 13).start()
        arrived(t, 6)
        outgoing(t, 14).start()

    def gather_d(t):
        arrived(t, 7)
        outgoing(t, 15).start()
        for e in range(8, 16):
            arrived(t, e)

    def entering(k, j):
        return pltpu.make_async_copy(
            hidden_hbm.at[k, 0, :, pl.ds(j * CW, CW)], inbox.at[k, j], hrecv.at[k, j]
        )

    for t in range(4):
        own_copy(t).start()

    @pl.when(s == 0)
    def _():
        for k in range(MICRO):
            for j in range(CHUNKS):
                entering(k, j).start()

    crossing_in = (s == 4) | (s == 0)
    crossing_out = (s == 3) | (s == SECTIONS - 1)
    before = (lax.rem(s + SECTIONS - 1, SECTIONS), jnp.where(crossing_in, mirrored, f))
    after_f = jnp.where(crossing_out, mirrored, f)
    barrier = pltpu.get_barrier_semaphore()
    greeted = [(s, dev_next), (s, dev_prev), (s, dev_x), (s, dev_sib), before]
    greeted.append((SECTIONS - 1, mirrored))
    for device in greeted:
        pl.semaphore_signal(barrier, inc=1, device_id=device, device_id_type=MESH)
    pl.semaphore_wait(barrier, 5 + jnp.where(s == SECTIONS - 1, SECTIONS, 0))

    gather_a(0)
    gather_a(1)
    gather_b(0)
    gather_b(1)
    gather_c(0)
    gather_a(2)
    gather_c(1)
    gather_a(3)
    gather_d(0)
    gather_d(1)

    def hop(k, j):
        last = s == SECTIONS - 1
        second = k >= MICRO
        to_section = jnp.where(last, jnp.where(second, k - MICRO, 0), s + 1)
        slot = jnp.where(last, jnp.where(second, FINAL, k + MICRO), k)
        return pltpu.make_async_remote_copy(
            src_ref=outbox.at[k, j],
            dst_ref=inbox.at[slot, j],
            send_sem=hsend.at[k, j],
            recv_sem=hrecv.at[slot, j],
            device_id=(to_section, after_f),
            device_id_type=MESH,
        )

    def hop_arrived(slot, j):
        pltpu.make_async_remote_copy(
            src_ref=inbox.at[slot, j],
            dst_ref=inbox.at[slot, j],
            send_sem=hsend.at[0, j],
            recv_sem=hrecv.at[slot, j],
            device_id=(s, dev_sib),
            device_id_type=MESH,
        ).wait_recv()

    def layer(k):
        c = lax.div(k, MICRO)
        squares = jnp.zeros((LEN, 128), jnp.float32)
        for j in range(CHUNKS):
            hop_arrived(k, j)
            wide = inbox[k, j].astype(jnp.float32)
            for p in range(CW // 128):
                part = wide[:, p * 128 : (p + 1) * 128]
                squares = squares + part * part
            scaled = (wide * gain_ref[c, :, j * CW : (j + 1) * CW]).astype(jnp.bfloat16)
            for n in range(QKV // 512):
                cols = slice(n * 512, (n + 1) * 512)
                product = jnp.dot(
                    scaled,
                    wq[c, j * CW : (j + 1) * CW, cols],
                    preferred_element_type=jnp.float32,
                )
                if j > 0:
                    product = product + acc[:, cols]
                acc[:, cols] = product
        inv = lax.rsqrt(jnp.sum(squares, axis=1, keepdims=True) * (1.0 / D) + EPS)

        def projected(col, width=HEAD_DIM):
            cols = slice(col, col + width)
            return acc[:, cols] * inv + bias_ref[c, :, cols]

        def rotated(value, table):
            turned = pltpu.roll(value, HEAD_DIM // 2, 1)
            return value * rope_ref[table] + turned * rope_ref[table + 1]

        for g in range(KV_HEADS):
            key_high, key_low = split_two(rotated(projected(D + g * HEAD_DIM), 2))
            value_rows = projected(D + (KV_HEADS + g) * HEAD_DIM).astype(jnp.bfloat16)
            heads = [
                split_two(rotated(projected((g * GROUP + h) * HEAD_DIM), 0))
                for h in range(GROUP)
            ]
            query_high = jnp.concatenate([h[0] for h in heads], axis=0)
            query_low = jnp.concatenate([h[1] for h in heads], axis=0)
            contract = (((1,), (1,)), ((), ()))
            scores = lax.dot_general(
                jnp.concatenate([query_high, query_low, query_high], axis=1),
                jnp.concatenate([key_high, key_high, key_low], axis=1),
                contract,
                preferred_element_type=jnp.float32,
            )
            scores = scores + jnp.concatenate([mask_ref[...]] * GROUP, axis=0)
            weights = jnp.exp(scores - jnp.max(scores, axis=1, keepdims=True))
            paired = jnp.concatenate([value_rows, jnp.ones_like(value_rows)], axis=1)
            mixed = jnp.dot(
                weights.astype(jnp.bfloat16), paired, preferred_element_type=jnp.float32
            )
            context = (mixed[:, :HEAD_DIM] / mixed[:, HEAD_DIM:]).astype(jnp.bfloat16)
            for h in range(GROUP):
                col = (g * GROUP + h) * HEAD_DIM
                ctx[:, col : col + HEAD_DIM] = context[h * LEN : (h + 1) * LEN]

        for j in range(CHUNKS):
            update = jnp.dot(
                ctx[...],
                wo[c, :, j * CW : (j + 1) * CW],
                preferred_element_type=jnp.float32,
            )
            outbox[k, j] = (inbox[k, j].astype(jnp.float32) + update).astype(jnp.bfloat16)
            hop(k, j).start()

    def step(k, carry):
        layer(k)

        @pl.when(k == 2)
        def _():
            gather_b(2)

        @pl.when(k == 3)
        def _():
            gather_b(3)

        @pl.when(k == 5)
        def _():
            gather_c(2)

        @pl.when(k == 6)
        def _():
            gather_c(3)

        @pl.when(k == 7)
        def _():
            gather_d(2)
            gather_d(3)

        return carry

    lax.fori_loop(0, STEPS, step, 0)

    for j in range(CHUNKS):
        hop_arrived(FINAL, j)
        result_ref[:, j * CW : (j + 1) * CW] = inbox[FINAL, j]

    def drain(k, carry):
        for j in range(CHUNKS):
            hop(k, j).wait_send()
        return carry

    lax.fori_loop(0, STEPS, drain, 0)
    for t in range(4):
        for e in range(EVENTS):
            outgoing(t, e).wait_send()


def per_device(hidden_in, norm_gain, qkv_weight, qkv_bias, out_weight):
    rope, mask = tables()
    vmem = pl.BlockSpec(memory_space=pltpu.VMEM)
    anywhere = pl.BlockSpec(memory_space=pl.ANY)
    dma = pltpu.SemaphoreType.DMA
    result = pl.pallas_call(
        kernel,
        name="sections",
        out_shape=jax.ShapeDtypeStruct((LEN, D), jnp.bfloat16),
        in_specs=[anywhere, vmem, anywhere, vmem, anywhere, vmem, vmem],
        out_specs=vmem,
        scratch_shapes=[
            pltpu.VMEM((2, D, QKV), jnp.bfloat16),
            pltpu.VMEM((2, D, D), jnp.bfloat16),
            pltpu.VMEM((STEPS + 1, CHUNKS, LEN, CW), jnp.bfloat16),
            pltpu.VMEM((STEPS, CHUNKS, LEN, CW), jnp.bfloat16),
            pltpu.VMEM((LEN, QKV), jnp.float32),
            pltpu.VMEM((LEN, D), jnp.bfloat16),
            dma((4,)),
            dma((4, EVENTS)),
            dma((4, EVENTS)),
            dma((STEPS, CHUNKS)),
            dma((STEPS + 1, CHUNKS)),
        ],
        compiler_params=pltpu.CompilerParams(collective_id=0, has_side_effects=True),
    )(hidden_in, norm_gain, qkv_weight, qkv_bias, out_weight, rope, mask)
    return result[None, None]


def solution(mesh):
    in_specs = (
        P(None, "fsdp", None, None),
        P(None, "section", None),
        P(None, "section", "fsdp", None),
        P(None, "section", None),
        P(None, "section", "fsdp", None),
    )
    out_specs = P("section", "fsdp", None, None)
    return jax.shard_map(
        per_device, mesh=mesh, in_specs=in_specs, out_specs=out_specs, check_vma=False
    )
```

```python
import functools
import math

import jax
import jax.numpy as jnp
import numpy as np
from jax import lax
from jax.experimental import pallas as pl
from jax.experimental.pallas import tpu as pltpu
from jax.sharding import PartitionSpec as P

HEADS = 12
KV_HEADS = 2
HEAD_DIM = 128
GROUP = HEADS // KV_HEADS
LEN = 64
PIECE = 32
PIECES = LEN // PIECE
D = HEADS * HEAD_DIM
QKV = D + 2 * KV_HEADS * HEAD_DIM
SECTIONS = 8
FSDP = 16
ROWS = D // FSDP
HALF = ROWS // 2
MICRO = 8
PASS = MICRO * PIECES
STEPS = 2 * PASS
CHUNKS = 3
CW = D // CHUNKS
FINAL = STEPS
THETA = 1000000.0
EPS = 1.0
EVENTS = 18
SLAB = 80
MESH = pl.DeviceIdType.MESH


def tables():
    frequency = np.exp(np.arange(HEAD_DIM // 2) * (-2.0 * math.log(THETA) / HEAD_DIM))
    angles = np.arange(LEN)[:, None] * frequency[None, :]
    cosine, sine = np.cos(angles), np.sin(angles)
    full_cos = np.concatenate([cosine, cosine], axis=1)
    full_sin = np.concatenate([-sine, sine], axis=1)
    scale = 1.0 / math.sqrt(HEAD_DIM)
    mask = np.where(np.arange(LEN)[:, None] >= np.arange(LEN)[None, :], 0.0, -1e30)
    rope = np.stack([full_cos * scale, full_sin * scale, full_cos, full_sin])
    rope = rope.reshape(4, PIECES, PIECE, HEAD_DIM).swapaxes(0, 1)
    mask = mask.reshape(PIECES, PIECE, LEN)
    return rope.astype(np.float32), mask.astype(np.float32)


def split_two(value):
    high = value.astype(jnp.bfloat16)
    low = (value - high.astype(jnp.float32)).astype(jnp.bfloat16)
    return high, low


def kernel(
    hidden_hbm,
    gain_ref,
    qkv_hbm,
    bias_ref,
    out_hbm,
    rope_ref,
    mask_ref,
    result_ref,
    wq,
    wo,
    inbox,
    outbox,
    acc,
    ctx,
    keys,
    values,
    own_sem,
    gsend,
    grecv,
    hsend,
    hrecv,
):
    s = lax.axis_index("section")
    f = lax.axis_index("fsdp")
    y = lax.div(f, 4)
    low = lax.rem(f, 4)
    x = lax.div(low, 2)
    core = lax.rem(f, 2)
    mirrored = f + 2 - 4 * x
    x_other = low + 2 - 4 * x
    y_next = lax.rem(y + 1, 4) * 4
    y_prev = lax.rem(y + 3, 4) * 4
    y_far = lax.rem(y + 2, 4) * 4
    flip = 1 - 2 * core

    dev_next = y_next + low
    dev_prev = y_prev + low
    dev_x = mirrored
    dev_sib = f + flip

    blocks = (
        f,
        y_prev + low,
        y_next + low,
        mirrored,
        y_far + low,
        y_prev + x_other,
        y_next + x_other,
        y_far + x_other,
    )
    OWN, PREV, NEXT, ACROSS, FAR, XPREV, XNEXT, XFAR = blocks

    tensors = ((wq, 0), (wo, 0), (wq, 1), (wo, 1))
    sources = ((qkv_hbm, 0), (out_hbm, 0), (qkv_hbm, 1), (out_hbm, 1))

    def region(t, block, first=0, count=ROWS):
        ref, layer = tensors[t]
        start = pl.multiple_of(block * ROWS + first, 16)
        return ref.at[layer, pl.ds(start, count), :]

    sends = {
        0: (OWN, 0, ROWS, dev_next),
        1: (OWN, 0, ROWS, dev_prev),
        2: (OWN, 0, ROWS, dev_x),
        3: (PREV, 0, HALF, dev_next),
        4: (NEXT, HALF, HALF, dev_prev),
        5: (ACROSS, 0, SLAB, dev_next),
        6: (ACROSS, 0, SLAB, dev_prev),
        7: (FAR, 0, ROWS, dev_x),
        16: (PREV, SLAB, ROWS - SLAB, dev_x),
        17: (NEXT, SLAB, ROWS - SLAB, dev_x),
    }
    lands = {
        0: (PREV, 0, ROWS),
        1: (NEXT, 0, ROWS),
        2: (ACROSS, 0, ROWS),
        3: (FAR, 0, HALF),
        4: (FAR, HALF, HALF),
        5: (XPREV, 0, SLAB),
        6: (XNEXT, 0, SLAB),
        7: (XFAR, 0, ROWS),
        16: (XPREV, SLAB, ROWS - SLAB),
        17: (XNEXT, SLAB, ROWS - SLAB),
    }
    for n in range(8):
        sends[8 + n] = (blocks[n], 0, ROWS, dev_sib)
        lands[8 + n] = (blocks[n] + flip, 0, ROWS)

    def outgoing(t, e):
        block, first, count, target = sends[e]
        part = region(t, block, first, count)
        return pltpu.make_async_remote_copy(
            src_ref=part,
            dst_ref=part,
            send_sem=gsend.at[t, e],
            recv_sem=grecv.at[t, e],
            device_id=(s, target),
            device_id_type=MESH,
        )

    def arrived(t, e):
        block, first, count = lands[e]
        part = region(t, block, first, count)
        pltpu.make_async_remote_copy(
            src_ref=part,
            dst_ref=part,
            send_sem=gsend.at[t, e],
            recv_sem=grecv.at[t, e],
            device_id=(s, dev_sib),
            device_id_type=MESH,
        ).wait_recv()

    def own_copy(t):
        ref, layer = sources[t]
        return pltpu.make_async_copy(ref.at[layer, 0], region(t, OWN), own_sem.at[t])

    def gather_a(t):
        own_copy(t).wait()
        for e in (0, 1, 2, 8):
            outgoing(t, e).start()

    def gather_b(t):
        for e, then in ((0, (3, 16, 9)), (1, (4, 17, 10))):
            arrived(t, e)
            for n in then:
                outgoing(t, n).start()

    def gather_c(t):
        arrived(t, 2)
        for n in (5, 6, 11):
            outgoing(t, n).start()

    def gather_d(t):
        arrived(t, 3)
        arrived(t, 4)
        for n in (7, 12):
            outgoing(t, n).start()

    def gather_e(t):
        for e, then in ((5, None), (16, 13), (6, None), (17, 14), (7, 15)):
            arrived(t, e)
            if then is not None:
                outgoing(t, then).start()

    def gather_f(t):
        for e in range(8, 16):
            arrived(t, e)

    def entering(k, j):
        return pltpu.make_async_copy(
            hidden_hbm.at[k // PIECES, 0, pl.ds(k % PIECES * PIECE, PIECE), pl.ds(j * CW, CW)],
            inbox.at[k, j],
            hrecv.at[k, j],
        )

    for t in range(4):
        own_copy(t).start()

    @pl.when(s == 0)
    def _():
        for k in range(PASS):
            for j in range(CHUNKS):
                entering(k, j).start()

    crossing_in = (s == 4) | (s == 0)
    crossing_out = (s == 3) | (s == SECTIONS - 1)
    before = (lax.rem(s + SECTIONS - 1, SECTIONS), jnp.where(crossing_in, mirrored, f))
    after_f = jnp.where(crossing_out, mirrored, f)
    barrier = pltpu.get_barrier_semaphore()
    greeted = [(s, dev_next), (s, dev_prev), (s, dev_x), (s, dev_sib), before]
    greeted.append((SECTIONS - 1, mirrored))
    for device in greeted:
        pl.semaphore_signal(barrier, inc=1, device_id=device, device_id_type=MESH)
    pl.semaphore_wait(barrier, 5 + jnp.where(s == SECTIONS - 1, SECTIONS, 0))

    gather_a(0)
    gather_a(1)
    keys[...] = jnp.zeros_like(keys)
    values[...] = jnp.ones_like(values)
    gather_b(0)
    gather_b(1)
    gather_c(0)
    gather_c(1)
    gather_d(0)
    gather_d(1)
    gather_e(0)
    gather_f(0)

    def settle():
        gather_e(1)
        gather_f(1)
        gather_a(2)
        gather_a(3)

    @pl.when(s > 0)
    def _():
        settle()

    def hop(k, j):
        last = s == SECTIONS - 1
        second = k >= PASS
        owner = lax.div(k, PIECES) - MICRO
        to_section = jnp.where(last, jnp.where(second, owner, 0), s + 1)
        slot = jnp.where(last, jnp.where(second, FINAL + lax.rem(k, PIECES), k + PASS), k)
        return pltpu.make_async_remote_copy(
            src_ref=outbox.at[k, j],
            dst_ref=inbox.at[slot, j],
            send_sem=hsend.at[k, j],
            recv_sem=hrecv.at[slot, j],
            device_id=(to_section, after_f),
            device_id_type=MESH,
        )

    def hop_arrived(slot, j):
        pltpu.make_async_remote_copy(
            src_ref=inbox.at[slot, j],
            dst_ref=inbox.at[slot, j],
            send_sem=hsend.at[0, j],
            recv_sem=hrecv.at[slot, j],
            device_id=(s, dev_sib),
            device_id_type=MESH,
        ).wait_recv()

    def layer(k):
        c = lax.div(k, PASS)
        piece = lax.rem(k, PIECES)
        squares = jnp.zeros((PIECE, 128), jnp.float32)
        for j in range(CHUNKS):
            hop_arrived(k, j)
            wide = inbox[k, j].astype(jnp.float32)
            for p in range(CW // 128):
                part = wide[:, p * 128 : (p + 1) * 128]
                squares = squares + part * part
            scaled = (wide * gain_ref[c, :, j * CW : (j + 1) * CW]).astype(jnp.bfloat16)
            for n in range(QKV // 512):
                cols = slice(n * 512, (n + 1) * 512)
                product = jnp.dot(
                    scaled,
                    wq[c, j * CW : (j + 1) * CW, cols],
                    preferred_element_type=jnp.float32,
                )
                if j > 0:
                    product = product + acc[:, cols]
                acc[:, cols] = product
        inv = lax.rsqrt(jnp.sum(squares, axis=1, keepdims=True) * (1.0 / D) + EPS)

        def projected(col, width=HEAD_DIM):
            cols = slice(col, col + width)
            return acc[:, cols] * inv + bias_ref[c, :, cols]

        def rotated(value, table):
            turned = pltpu.roll(value, HEAD_DIM // 2, 1)
            return value * rope_ref[piece, table] + turned * rope_ref[piece, table + 1]

        rows = pl.ds(pl.multiple_of(piece * PIECE, PIECE), PIECE)
        for g in range(KV_HEADS):
            key_high, key_low = split_two(rotated(projected(D + g * HEAD_DIM), 2))
            keys[g, rows, :HEAD_DIM] = key_high
            keys[g, rows, HEAD_DIM:] = key_low
            value_rows = projected(D + (KV_HEADS + g) * HEAD_DIM)
            values[g, rows, :HEAD_DIM] = value_rows.astype(jnp.bfloat16)
        for g in range(KV_HEADS):
            heads = [
                split_two(rotated(projected((g * GROUP + h) * HEAD_DIM), 0))
                for h in range(GROUP)
            ]
            query_high = jnp.concatenate([h[0] for h in heads], axis=0)
            query_low = jnp.concatenate([h[1] for h in heads], axis=0)
            key_high = keys[g, :, :HEAD_DIM]
            key_low = keys[g, :, HEAD_DIM:]
            contract = (((1,), (1,)), ((), ()))
            scores = lax.dot_general(
                jnp.concatenate([query_high, query_low, query_high], axis=1),
                jnp.concatenate([key_high, key_high, key_low], axis=1),
                contract,
                preferred_element_type=jnp.float32,
            )
            scores = scores + jnp.concatenate([mask_ref[piece]] * GROUP, axis=0)
            weights = jnp.exp(scores - jnp.max(scores, axis=1, keepdims=True))
            mixed = jnp.dot(
                weights.astype(jnp.bfloat16), values[g], preferred_element_type=jnp.float32
            )
            context = (mixed[:, :HEAD_DIM] / mixed[:, HEAD_DIM:]).astype(jnp.bfloat16)
            for h in range(GROUP):
                col = (g * GROUP + h) * HEAD_DIM
                ctx[:, col : col + HEAD_DIM] = context[h * PIECE : (h + 1) * PIECE]

        @pl.when((k == 0) & (s == 0))
        def _():
            settle()

        for j in range(CHUNKS):
            update = jnp.dot(
                ctx[...],
                wo[c, :, j * CW : (j + 1) * CW],
                preferred_element_type=jnp.float32,
            )
            outbox[k, j] = (inbox[k, j].astype(jnp.float32) + update).astype(jnp.bfloat16)
            hop(k, j).start()

    def step(k, carry):
        layer(k)

        @pl.when(k == 4)
        def _():
            gather_b(2)

        @pl.when(k == 7)
        def _():
            gather_b(3)
            gather_c(2)
            gather_c(3)

        @pl.when(k == 9)
        def _():
            gather_d(2)
            gather_d(3)

        @pl.when(k == 15)
        def _():
            for t in (2, 3):
                gather_e(t)
                gather_f(t)

        return carry

    lax.fori_loop(0, STEPS, step, 0)

    for n in range(PIECES):
        for j in range(CHUNKS):
            hop_arrived(FINAL + n, j)
            result_ref[n * PIECE : (n + 1) * PIECE, j * CW : (j + 1) * CW] = inbox[FINAL + n, j]

    def drain(k, carry):
        for j in range(CHUNKS):
            hop(k, j).wait_send()
        return carry

    lax.fori_loop(0, STEPS, drain, 0)
    for t in range(4):
        for e in range(EVENTS):
            outgoing(t, e).wait_send()


def per_device(hidden_in, norm_gain, qkv_weight, qkv_bias, out_weight):
    rope, mask = tables()
    vmem = pl.BlockSpec(memory_space=pltpu.VMEM)
    anywhere = pl.BlockSpec(memory_space=pl.ANY)
    dma = pltpu.SemaphoreType.DMA
    result = pl.pallas_call(
        kernel,
        name="sections",
        out_shape=jax.ShapeDtypeStruct((LEN, D), jnp.bfloat16),
        in_specs=[anywhere, vmem, anywhere, vmem, anywhere, vmem, vmem],
        out_specs=vmem,
        scratch_shapes=[
            pltpu.VMEM((2, D, QKV), jnp.bfloat16),
            pltpu.VMEM((2, D, D), jnp.bfloat16),
            pltpu.VMEM((STEPS + PIECES, CHUNKS, PIECE, CW), jnp.bfloat16),
            pltpu.VMEM((STEPS, CHUNKS, PIECE, CW), jnp.bfloat16),
            pltpu.VMEM((PIECE, QKV), jnp.float32),
            pltpu.VMEM((PIECE, D), jnp.bfloat16),
            pltpu.VMEM((KV_HEADS, LEN, 2 * HEAD_DIM), jnp.bfloat16),
            pltpu.VMEM((KV_HEADS, LEN, 2 * HEAD_DIM), jnp.bfloat16),
            dma((4,)),
            dma((4, EVENTS)),
            dma((4, EVENTS)),
            dma((STEPS, CHUNKS)),
            dma((STEPS + PIECES, CHUNKS)),
        ],
        compiler_params=pltpu.CompilerParams(collective_id=0, has_side_effects=True),
    )(hidden_in, norm_gain, qkv_weight, qkv_bias, out_weight, rope, mask)
    return result[None, None]


def solution(mesh):
    in_specs = (
        P(None, "fsdp", None, None),
        P(None, "section", None),
        P(None, "section", "fsdp", None),
        P(None, "section", None),
        P(None, "section", "fsdp", None),
    )
    out_specs = P("section", "fsdp", None, None)
    return jax.shard_map(
        per_device, mesh=mesh, in_specs=in_specs, out_specs=out_specs, check_vma=False
    )
```

```python
import functools
import math

import jax
import jax.numpy as jnp
import numpy as np
from jax import lax
from jax.experimental import pallas as pl
from jax.experimental.pallas import tpu as pltpu
from jax.sharding import PartitionSpec as P

HEADS = 12
KV_HEADS = 2
HEAD_DIM = 128
GROUP = HEADS // KV_HEADS
LEN = 64
PIECE = 32
PIECES = LEN // PIECE
D = HEADS * HEAD_DIM
QKV = D + 2 * KV_HEADS * HEAD_DIM
SECTIONS = 8
FSDP = 16
ROWS = D // FSDP
HALF = ROWS // 2
MICRO = 8
PASS = MICRO * PIECES
STEPS = 2 * PASS
CHUNKS = 3
CW = D // CHUNKS
FINAL = STEPS
THETA = 1000000.0
EPS = 1.0
EVENTS = 18
SLAB = 80
MESH = pl.DeviceIdType.MESH


def tables():
    frequency = np.exp(np.arange(HEAD_DIM // 2) * (-2.0 * math.log(THETA) / HEAD_DIM))
    angles = np.arange(LEN)[:, None] * frequency[None, :]
    cosine, sine = np.cos(angles), np.sin(angles)
    full_cos = np.concatenate([cosine, cosine], axis=1)
    full_sin = np.concatenate([-sine, sine], axis=1)
    scale = 1.0 / math.sqrt(HEAD_DIM)
    mask = np.where(np.arange(LEN)[:, None] >= np.arange(LEN)[None, :], 0.0, -1e30)
    rope = np.stack([full_cos * scale, full_sin * scale, full_cos, full_sin])
    rope = rope.reshape(4, PIECES, PIECE, HEAD_DIM).swapaxes(0, 1)
    mask = mask.reshape(PIECES, PIECE, LEN)
    return rope.astype(np.float32), mask.astype(np.float32)


def split_two(value):
    high = value.astype(jnp.bfloat16)
    low = (value - high.astype(jnp.float32)).astype(jnp.bfloat16)
    return high, low


def kernel(
    hidden_hbm,
    gain_ref,
    qkv_hbm,
    bias_ref,
    out_hbm,
    rope_ref,
    mask_ref,
    result_ref,
    wq,
    wo,
    inbox,
    outbox,
    acc,
    keys,
    values,
    own_sem,
    gsend,
    grecv,
    hsend,
    hrecv,
):
    s = lax.axis_index("section")
    f = lax.axis_index("fsdp")
    y = lax.div(f, 4)
    low = lax.rem(f, 4)
    x = lax.div(low, 2)
    core = lax.rem(f, 2)
    mirrored = f + 2 - 4 * x
    x_other = low + 2 - 4 * x
    y_next = lax.rem(y + 1, 4) * 4
    y_prev = lax.rem(y + 3, 4) * 4
    y_far = lax.rem(y + 2, 4) * 4
    flip = 1 - 2 * core

    dev_next = y_next + low
    dev_prev = y_prev + low
    dev_x = mirrored
    dev_sib = f + flip

    blocks = (
        f,
        y_prev + low,
        y_next + low,
        mirrored,
        y_far + low,
        y_prev + x_other,
        y_next + x_other,
        y_far + x_other,
    )
    OWN, PREV, NEXT, ACROSS, FAR, XPREV, XNEXT, XFAR = blocks

    tensors = ((wq, 0), (wo, 0), (wq, 1), (wo, 1))
    sources = ((qkv_hbm, 0), (out_hbm, 0), (qkv_hbm, 1), (out_hbm, 1))

    def region(t, block, first=0, count=ROWS):
        ref, layer = tensors[t]
        start = pl.multiple_of(block * ROWS + first, 16)
        return ref.at[layer, pl.ds(start, count), :]

    sends = {
        0: (OWN, 0, ROWS, dev_next),
        1: (OWN, 0, ROWS, dev_prev),
        2: (OWN, 0, ROWS, dev_x),
        3: (PREV, 0, HALF, dev_next),
        4: (NEXT, HALF, HALF, dev_prev),
        5: (ACROSS, 0, SLAB, dev_next),
        6: (ACROSS, 0, SLAB, dev_prev),
        7: (FAR, 0, ROWS, dev_x),
        16: (PREV, SLAB, ROWS - SLAB, dev_x),
        17: (NEXT, SLAB, ROWS - SLAB, dev_x),
    }
    lands = {
        0: (PREV, 0, ROWS),
        1: (NEXT, 0, ROWS),
        2: (ACROSS, 0, ROWS),
        3: (FAR, 0, HALF),
        4: (FAR, HALF, HALF),
        5: (XPREV, 0, SLAB),
        6: (XNEXT, 0, SLAB),
        7: (XFAR, 0, ROWS),
        16: (XPREV, SLAB, ROWS - SLAB),
        17: (XNEXT, SLAB, ROWS - SLAB),
    }
    for n in range(8):
        sends[8 + n] = (blocks[n], 0, ROWS, dev_sib)
        lands[8 + n] = (blocks[n] + flip, 0, ROWS)

    def outgoing(t, e):
        block, first, count, target = sends[e]
        part = region(t, block, first, count)
        return pltpu.make_async_remote_copy(
            src_ref=part,
            dst_ref=part,
            send_sem=gsend.at[t, e],
            recv_sem=grecv.at[t, e],
            device_id=(s, target),
            device_id_type=MESH,
        )

    def arrived(t, e):
        block, first, count = lands[e]
        part = region(t, block, first, count)
        pltpu.make_async_remote_copy(
            src_ref=part,
            dst_ref=part,
            send_sem=gsend.at[t, e],
            recv_sem=grecv.at[t, e],
            device_id=(s, dev_sib),
            device_id_type=MESH,
        ).wait_recv()

    def own_copy(t):
        ref, layer = sources[t]
        return pltpu.make_async_copy(ref.at[layer, 0], region(t, OWN), own_sem.at[t])

    def gather_a(t):
        own_copy(t).wait()
        for e in (0, 1, 2, 8):
            outgoing(t, e).start()

    def gather_b(t):
        for e, then in ((0, (3, 16, 9)), (1, (4, 17, 10))):
            arrived(t, e)
            for n in then:
                outgoing(t, n).start()

    def gather_c(t):
        arrived(t, 2)
        for n in (5, 6, 11):
            outgoing(t, n).start()

    def gather_d(t):
        arrived(t, 3)
        arrived(t, 4)
        for n in (7, 12):
            outgoing(t, n).start()

    def gather_e(t):
        for e, then in ((5, None), (16, 13), (6, None), (17, 14), (7, 15)):
            arrived(t, e)
            if then is not None:
                outgoing(t, then).start()

    def gather_f(t):
        for e in range(8, 16):
            arrived(t, e)

    def entering(k, j):
        return pltpu.make_async_copy(
            hidden_hbm.at[k // PIECES, 0, pl.ds(k % PIECES * PIECE, PIECE), pl.ds(j * CW, CW)],
            inbox.at[k, j],
            hrecv.at[k, j],
        )

    for t in range(4):
        own_copy(t).start()

    @pl.when(s == 0)
    def _():
        for k in range(PASS):
            for j in range(CHUNKS):
                entering(k, j).start()

    crossing_in = (s == 4) | (s == 0)
    crossing_out = (s == 3) | (s == SECTIONS - 1)
    before = (lax.rem(s + SECTIONS - 1, SECTIONS), jnp.where(crossing_in, mirrored, f))
    after_f = jnp.where(crossing_out, mirrored, f)
    barrier = pltpu.get_barrier_semaphore()
    greeted = [(s, dev_next), (s, dev_prev), (s, dev_x), (s, dev_sib), before]
    greeted.append((SECTIONS - 1, mirrored))
    for device in greeted:
        pl.semaphore_signal(barrier, inc=1, device_id=device, device_id_type=MESH)
    pl.semaphore_wait(barrier, 5 + jnp.where(s == SECTIONS - 1, SECTIONS, 0))

    gather_a(0)
    gather_a(1)
    keys[...] = jnp.zeros_like(keys)
    values[...] = jnp.ones_like(values)
    gather_b(0)
    gather_b(1)
    gather_c(0)
    gather_c(1)
    gather_d(0)
    gather_d(1)
    gather_e(0)
    gather_f(0)

    gather_e(1)
    gather_f(1)
    gather_a(2)
    gather_a(3)

    def hop(k, j):
        last = s == SECTIONS - 1
        second = k >= PASS
        owner = lax.div(k, PIECES) - MICRO
        to_section = jnp.where(last, jnp.where(second, owner, 0), s + 1)
        slot = jnp.where(last, jnp.where(second, FINAL + lax.rem(k, PIECES), k + PASS), k)
        return pltpu.make_async_remote_copy(
            src_ref=outbox.at[k, j],
            dst_ref=inbox.at[slot, j],
            send_sem=hsend.at[k, j],
            recv_sem=hrecv.at[slot, j],
            device_id=(to_section, after_f),
            device_id_type=MESH,
        )

    def hop_arrived(slot, j):
        pltpu.make_async_remote_copy(
            src_ref=inbox.at[slot, j],
            dst_ref=inbox.at[slot, j],
            send_sem=hsend.at[0, j],
            recv_sem=hrecv.at[slot, j],
            device_id=(s, dev_sib),
            device_id_type=MESH,
        ).wait_recv()

    def layer(k):
        c = lax.div(k, PASS)
        piece = lax.rem(k, PIECES)
        squares = jnp.zeros((PIECE, 128), jnp.float32)
        for j in range(CHUNKS):
            hop_arrived(k, j)
            wide = inbox[k, j].astype(jnp.float32)
            for p in range(CW // 128):
                part = wide[:, p * 128 : (p + 1) * 128]
                squares = squares + part * part
            scaled = (wide * gain_ref[c, :, j * CW : (j + 1) * CW]).astype(jnp.bfloat16)
            for n in (3, 0, 1, 2):
                cols = slice(n * 512, (n + 1) * 512)
                product = jnp.dot(
                    scaled,
                    wq[c, j * CW : (j + 1) * CW, cols],
                    preferred_element_type=jnp.float32,
                )
                if j > 0:
                    product = product + acc[:, cols]
                acc[:, cols] = product
        inv = lax.rsqrt(jnp.sum(squares, axis=1, keepdims=True) * (1.0 / D) + EPS)

        def projected(col, width=HEAD_DIM):
            cols = slice(col, col + width)
            return acc[:, cols] * inv + bias_ref[c, :, cols]

        def rotated(value, table):
            turned = pltpu.roll(value, HEAD_DIM // 2, 1)
            return value * rope_ref[piece, table] + turned * rope_ref[piece, table + 1]

        rows = pl.ds(pl.multiple_of(piece * PIECE, PIECE), PIECE)
        for g in range(KV_HEADS):
            key_high, key_low = split_two(rotated(projected(D + g * HEAD_DIM), 2))
            keys[g, rows, :HEAD_DIM] = key_high
            keys[g, rows, HEAD_DIM:] = key_low
            value_rows = projected(D + (KV_HEADS + g) * HEAD_DIM)
            values[g, rows, :HEAD_DIM] = value_rows.astype(jnp.bfloat16)
        half = GROUP * HEAD_DIM
        updates = [None] * CHUNKS
        for g in range(KV_HEADS):
            heads = [
                split_two(rotated(projected((g * GROUP + h) * HEAD_DIM), 0))
                for h in range(GROUP)
            ]
            query_high = jnp.concatenate([h[0] for h in heads], axis=0)
            query_low = jnp.concatenate([h[1] for h in heads], axis=0)
            key_high = keys[g, :, :HEAD_DIM]
            key_low = keys[g, :, HEAD_DIM:]
            contract = (((1,), (1,)), ((), ()))
            scores = lax.dot_general(
                jnp.concatenate([query_high, query_low, query_high], axis=1),
                jnp.concatenate([key_high, key_high, key_low], axis=1),
                contract,
                preferred_element_type=jnp.float32,
            )
            scores = scores + jnp.concatenate([mask_ref[piece]] * GROUP, axis=0)
            weights = jnp.exp(scores - jnp.max(scores, axis=1, keepdims=True))
            mixed = jnp.dot(
                weights.astype(jnp.bfloat16), values[g], preferred_element_type=jnp.float32
            )
            context = (mixed[:, :HEAD_DIM] / mixed[:, HEAD_DIM:]).astype(jnp.bfloat16)
            context = jnp.concatenate(
                [context[h * PIECE : (h + 1) * PIECE] for h in range(GROUP)], axis=1
            )

            def finish(j):
                total = inbox[k, j].astype(jnp.float32) + updates[j]
                outbox[k, j] = total.astype(jnp.bfloat16)
                hop(k, j).start()

            for j in range(CHUNKS):
                product = jnp.dot(
                    context,
                    wo[c, g * half : (g + 1) * half, j * CW : (j + 1) * CW],
                    preferred_element_type=jnp.float32,
                )
                updates[j] = product if g == 0 else updates[j] + product
                if g > 0 and j > 0:
                    finish(j - 1)
        finish(CHUNKS - 1)

    def step(k, carry):
        layer(k)

        @pl.when(k == 4)
        def _():
            gather_b(2)

        @pl.when(k == 7)
        def _():
            gather_b(3)
            gather_c(2)
            gather_c(3)

        @pl.when(k == 9)
        def _():
            gather_d(2)
            gather_d(3)

        @pl.when(k == 15)
        def _():
            for t in (2, 3):
                gather_e(t)
                gather_f(t)

        return carry

    lax.fori_loop(0, STEPS, step, 0)

    for n in range(PIECES):
        for j in range(CHUNKS):
            hop_arrived(FINAL + n, j)
            result_ref[n * PIECE : (n + 1) * PIECE, j * CW : (j + 1) * CW] = inbox[FINAL + n, j]

    def drain(k, carry):
        for j in range(CHUNKS):
            hop(k, j).wait_send()
        return carry

    lax.fori_loop(0, STEPS, drain, 0)
    for t in range(4):
        for e in range(EVENTS):
            outgoing(t, e).wait_send()


def per_device(hidden_in, norm_gain, qkv_weight, qkv_bias, out_weight):
    rope, mask = tables()
    vmem = pl.BlockSpec(memory_space=pltpu.VMEM)
    anywhere = pl.BlockSpec(memory_space=pl.ANY)
    dma = pltpu.SemaphoreType.DMA
    result = pl.pallas_call(
        kernel,
        name="sections",
        out_shape=jax.ShapeDtypeStruct((LEN, D), jnp.bfloat16),
        in_specs=[anywhere, vmem, anywhere, vmem, anywhere, vmem, vmem],
        out_specs=vmem,
        scratch_shapes=[
            pltpu.VMEM((2, D, QKV), jnp.bfloat16),
            pltpu.VMEM((2, D, D), jnp.bfloat16),
            pltpu.VMEM((STEPS + PIECES, CHUNKS, PIECE, CW), jnp.bfloat16),
            pltpu.VMEM((STEPS, CHUNKS, PIECE, CW), jnp.bfloat16),
            pltpu.VMEM((PIECE, QKV), jnp.float32),
            pltpu.VMEM((KV_HEADS, LEN, 2 * HEAD_DIM), jnp.bfloat16),
            pltpu.VMEM((KV_HEADS, LEN, 2 * HEAD_DIM), jnp.bfloat16),
            dma((4,)),
            dma((4, EVENTS)),
            dma((4, EVENTS)),
            dma((STEPS, CHUNKS)),
            dma((STEPS + PIECES, CHUNKS)),
        ],
        compiler_params=pltpu.CompilerParams(collective_id=0, has_side_effects=True),
    )(hidden_in, norm_gain, qkv_weight, qkv_bias, out_weight, rope, mask)
    return result[None, None]


def solution(mesh):
    in_specs = (
        P(None, "fsdp", None, None),
        P(None, "section", None),
        P(None, "section", "fsdp", None),
        P(None, "section", None),
        P(None, "section", "fsdp", None),
    )
    out_specs = P("section", "fsdp", None, None)
    return jax.shard_map(
        per_device, mesh=mesh, in_specs=in_specs, out_specs=out_specs, check_vma=False
    )
```

```python
import functools
import math

import jax
import jax.numpy as jnp
import numpy as np
from jax import lax
from jax.experimental import pallas as pl
from jax.experimental.pallas import tpu as pltpu
from jax.sharding import PartitionSpec as P

HEADS = 12
KV_HEADS = 2
HEAD_DIM = 128
GROUP = HEADS // KV_HEADS
LEN = 64
PIECE = 32
PIECES = LEN // PIECE
D = HEADS * HEAD_DIM
QKV = D + 2 * KV_HEADS * HEAD_DIM
SECTIONS = 8
FSDP = 16
ROWS = D // FSDP
HALF = ROWS // 2
MICRO = 8
PASS = MICRO * PIECES
STEPS = 2 * PASS
CHUNKS = 3
CW = D // CHUNKS
FINAL = STEPS
THETA = 1000000.0
EPS = 1.0
EVENTS = 18
SLAB = 80
MESH = pl.DeviceIdType.MESH


def tables():
    frequency = np.exp(np.arange(HEAD_DIM // 2) * (-2.0 * math.log(THETA) / HEAD_DIM))
    angles = np.arange(LEN)[:, None] * frequency[None, :]
    cosine, sine = np.cos(angles), np.sin(angles)
    full_cos = np.concatenate([cosine, cosine], axis=1)
    full_sin = np.concatenate([-sine, sine], axis=1)
    scale = 1.0 / math.sqrt(HEAD_DIM)
    mask = np.where(np.arange(LEN)[:, None] >= np.arange(LEN)[None, :], 0.0, -1e30)
    rope = np.stack([full_cos * scale, full_sin * scale, full_cos, full_sin])
    rope = rope.reshape(4, PIECES, PIECE, HEAD_DIM).swapaxes(0, 1)
    mask = mask.reshape(PIECES, PIECE, LEN)
    return rope.astype(np.float32), mask.astype(np.float32)


def split_two(value):
    high = value.astype(jnp.bfloat16)
    low = (value - high.astype(jnp.float32)).astype(jnp.bfloat16)
    return high, low


def kernel(
    hidden_hbm,
    gain_ref,
    qkv_hbm,
    bias_ref,
    out_hbm,
    rope_ref,
    mask_ref,
    result_ref,
    wq,
    wo,
    inbox,
    outbox,
    acc,
    keys,
    values,
    own_sem,
    gsend,
    grecv,
    hsend,
    hrecv,
):
    s = lax.axis_index("section")
    f = lax.axis_index("fsdp")
    y = lax.div(f, 4)
    low = lax.rem(f, 4)
    x = lax.div(low, 2)
    core = lax.rem(f, 2)
    mirrored = f + 2 - 4 * x
    x_other = low + 2 - 4 * x
    y_next = lax.rem(y + 1, 4) * 4
    y_prev = lax.rem(y + 3, 4) * 4
    y_far = lax.rem(y + 2, 4) * 4
    flip = 1 - 2 * core

    dev_next = y_next + low
    dev_prev = y_prev + low
    dev_x = mirrored
    dev_sib = f + flip

    blocks = (
        f,
        y_prev + low,
        y_next + low,
        mirrored,
        y_far + low,
        y_prev + x_other,
        y_next + x_other,
        y_far + x_other,
    )
    OWN, PREV, NEXT, ACROSS, FAR, XPREV, XNEXT, XFAR = blocks

    tensors = ((wq, 0), (wo, 0), (wq, 1), (wo, 1))
    sources = ((qkv_hbm, 0), (out_hbm, 0), (qkv_hbm, 1), (out_hbm, 1))

    def region(t, block, first=0, count=ROWS):
        ref, layer = tensors[t]
        start = pl.multiple_of(block * ROWS + first, 16)
        return ref.at[layer, pl.ds(start, count), :]

    sends = {
        0: (OWN, 0, ROWS, dev_next),
        1: (OWN, 0, ROWS, dev_prev),
        2: (OWN, 0, ROWS, dev_x),
        3: (PREV, 0, HALF, dev_next),
        4: (NEXT, HALF, HALF, dev_prev),
        5: (ACROSS, 0, SLAB, dev_next),
        6: (ACROSS, 0, SLAB, dev_prev),
        7: (FAR, 0, ROWS, dev_x),
        16: (PREV, SLAB, ROWS - SLAB, dev_x),
        17: (NEXT, SLAB, ROWS - SLAB, dev_x),
    }
    lands = {
        0: (PREV, 0, ROWS),
        1: (NEXT, 0, ROWS),
        2: (ACROSS, 0, ROWS),
        3: (FAR, 0, HALF),
        4: (FAR, HALF, HALF),
        5: (XPREV, 0, SLAB),
        6: (XNEXT, 0, SLAB),
        7: (XFAR, 0, ROWS),
        16: (XPREV, SLAB, ROWS - SLAB),
        17: (XNEXT, SLAB, ROWS - SLAB),
    }
    for n in range(8):
        sends[8 + n] = (blocks[n], 0, ROWS, dev_sib)
        lands[8 + n] = (blocks[n] + flip, 0, ROWS)

    def outgoing(t, e):
        block, first, count, target = sends[e]
        part = region(t, block, first, count)
        return pltpu.make_async_remote_copy(
            src_ref=part,
            dst_ref=part,
            send_sem=gsend.at[t, e],
            recv_sem=grecv.at[t, e],
            device_id=(s, target),
            device_id_type=MESH,
        )

    def arrived(t, e):
        block, first, count = lands[e]
        part = region(t, block, first, count)
        pltpu.make_async_remote_copy(
            src_ref=part,
            dst_ref=part,
            send_sem=gsend.at[t, e],
            recv_sem=grecv.at[t, e],
            device_id=(s, dev_sib),
            device_id_type=MESH,
        ).wait_recv()

    def own_copy(t):
        ref, layer = sources[t]
        return pltpu.make_async_copy(ref.at[layer, 0], region(t, OWN), own_sem.at[t])

    def gather_a(t):
        own_copy(t).wait()
        for e in (0, 1, 2, 8):
            outgoing(t, e).start()

    def gather_b(t):
        for e, then in ((0, (3, 16, 9)), (1, (4, 17, 10))):
            arrived(t, e)
            for n in then:
                outgoing(t, n).start()

    def gather_c(t):
        arrived(t, 2)
        for n in (5, 6, 11):
            outgoing(t, n).start()

    def gather_d(t):
        arrived(t, 3)
        arrived(t, 4)
        for n in (7, 12):
            outgoing(t, n).start()

    def gather_e(t):
        for e, then in ((5, None), (16, 13), (6, None), (17, 14), (7, 15)):
            arrived(t, e)
            if then is not None:
                outgoing(t, then).start()

    def gather_f(t):
        for e in range(8, 16):
            arrived(t, e)

    def entering(k, j):
        return pltpu.make_async_copy(
            hidden_hbm.at[k // PIECES, 0, pl.ds(k % PIECES * PIECE, PIECE), pl.ds(j * CW, CW)],
            inbox.at[k, j],
            hrecv.at[k, j],
        )

    for t in range(4):
        own_copy(t).start()

    @pl.when(s == 0)
    def _():
        for k in range(PASS):
            for j in range(CHUNKS):
                entering(k, j).start()

    crossing_in = (s == 4) | (s == 0)
    crossing_out = (s == 3) | (s == SECTIONS - 1)
    before = (lax.rem(s + SECTIONS - 1, SECTIONS), jnp.where(crossing_in, mirrored, f))
    after_f = jnp.where(crossing_out, mirrored, f)
    barrier = pltpu.get_barrier_semaphore()
    greeted = [(s, dev_next), (s, dev_prev), (s, dev_x), (s, dev_sib), before]
    greeted.append((SECTIONS - 1, mirrored))
    for device in greeted:
        pl.semaphore_signal(barrier, inc=1, device_id=device, device_id_type=MESH)
    pl.semaphore_wait(barrier, 5 + jnp.where(s == SECTIONS - 1, SECTIONS, 0))

    gather_a(0)
    gather_a(1)
    keys[...] = jnp.zeros_like(keys)
    values[...] = jnp.ones_like(values)
    gather_b(0)
    gather_b(1)
    gather_c(0)
    gather_c(1)
    gather_d(0)
    gather_d(1)
    gather_e(0)
    gather_f(0)

    gather_e(1)
    gather_f(1)
    gather_a(2)
    gather_a(3)

    def hop(k, j):
        last = s == SECTIONS - 1
        second = k >= PASS
        owner = lax.div(k, PIECES) - MICRO
        to_section = jnp.where(last, jnp.where(second, owner, 0), s + 1)
        slot = jnp.where(last, jnp.where(second, FINAL + lax.rem(k, PIECES), k + PASS), k)
        return pltpu.make_async_remote_copy(
            src_ref=outbox.at[k, j],
            dst_ref=inbox.at[slot, j],
            send_sem=hsend.at[k, j],
            recv_sem=hrecv.at[slot, j],
            device_id=(to_section, after_f),
            device_id_type=MESH,
        )

    def hop_arrived(slot, j):
        pltpu.make_async_remote_copy(
            src_ref=inbox.at[slot, j],
            dst_ref=inbox.at[slot, j],
            send_sem=hsend.at[0, j],
            recv_sem=hrecv.at[slot, j],
            device_id=(s, dev_sib),
            device_id_type=MESH,
        ).wait_recv()

    def layer(k):
        c = lax.div(k, PASS)
        piece = lax.rem(k, PIECES)
        squares = jnp.zeros((PIECE, 128), jnp.float32)
        for j in range(CHUNKS):
            hop_arrived(k, j)
            wide = inbox[k, j].astype(jnp.float32)
            for p in range(CW // 128):
                part = wide[:, p * 128 : (p + 1) * 128]
                squares = squares + part * part
            scaled = (wide * gain_ref[c, :, j * CW : (j + 1) * CW]).astype(jnp.bfloat16)
            for n in (3, 0, 1, 2):
                cols = slice(n * 512, (n + 1) * 512)
                product = jnp.dot(
                    scaled,
                    wq[c, j * CW : (j + 1) * CW, cols],
                    preferred_element_type=jnp.float32,
                )
                if j > 0:
                    product = product + acc[:, cols]
                acc[:, cols] = product
        inv = lax.rsqrt(jnp.sum(squares, axis=1, keepdims=True) * (1.0 / D) + EPS)

        def projected(col, width=HEAD_DIM):
            cols = slice(col, col + width)
            return acc[:, cols] * inv + bias_ref[c, :, cols]

        def rotated(value, table):
            turned = pltpu.roll(value, HEAD_DIM // 2, 1)
            return value * rope_ref[piece, table] + turned * rope_ref[piece, table + 1]

        rows = pl.ds(pl.multiple_of(piece * PIECE, PIECE), PIECE)
        for g in range(KV_HEADS):
            key_high, key_low = split_two(rotated(projected(D + g * HEAD_DIM), 2))
            keys[g, rows, :HEAD_DIM] = key_high
            keys[g, rows, HEAD_DIM:] = key_low
            value_rows = projected(D + (KV_HEADS + g) * HEAD_DIM)
            values[g, rows, :HEAD_DIM] = value_rows.astype(jnp.bfloat16)
        contract = (((1,), (1,)), ((), ()))
        mask = jnp.concatenate([mask_ref[piece]] * GROUP, axis=0)
        scores = []
        for g in range(KV_HEADS):
            heads = [
                split_two(rotated(projected((g * GROUP + h) * HEAD_DIM), 0))
                for h in range(GROUP)
            ]
            query_high = jnp.concatenate([h[0] for h in heads], axis=0)
            query_low = jnp.concatenate([h[1] for h in heads], axis=0)
            key_high = keys[g, :, :HEAD_DIM]
            key_low = keys[g, :, HEAD_DIM:]
            scores.append(
                lax.dot_general(
                    jnp.concatenate([query_high, query_low, query_high], axis=1),
                    jnp.concatenate([key_high, key_high, key_low], axis=1),
                    contract,
                    preferred_element_type=jnp.float32,
                )
            )
        weights = []
        for g in range(KV_HEADS):
            masked = scores[g] + mask
            shifted = masked - jnp.max(masked, axis=1, keepdims=True)
            weights.append(jnp.exp(shifted).astype(jnp.bfloat16))
        mixed = [
            jnp.dot(weights[g], values[g], preferred_element_type=jnp.float32)
            for g in range(KV_HEADS)
        ]
        contexts = []
        for g in range(KV_HEADS):
            context = (mixed[g][:, :HEAD_DIM] / mixed[g][:, HEAD_DIM:]).astype(jnp.bfloat16)
            contexts.append(
                jnp.concatenate(
                    [context[h * PIECE : (h + 1) * PIECE] for h in range(GROUP)], axis=1
                )
            )

        updates = [None] * CHUNKS
        half = GROUP * HEAD_DIM

        def finish(j):
            total = inbox[k, j].astype(jnp.float32) + updates[j]
            outbox[k, j] = total.astype(jnp.bfloat16)
            hop(k, j).start()

        for j in range(CHUNKS):
            for g in range(KV_HEADS):
                product = jnp.dot(
                    contexts[g],
                    wo[c, g * half : (g + 1) * half, j * CW : (j + 1) * CW],
                    preferred_element_type=jnp.float32,
                )
                updates[j] = product if g == 0 else updates[j] + product
            if j > 0:
                finish(j - 1)
        finish(CHUNKS - 1)

    def step(k, carry):
        layer(k)

        @pl.when(k == 4)
        def _():
            gather_b(2)

        @pl.when(k == 7)
        def _():
            gather_b(3)
            gather_c(2)
            gather_c(3)

        @pl.when(k == 9)
        def _():
            gather_d(2)
            gather_d(3)

        @pl.when(k == 15)
        def _():
            for t in (2, 3):
                gather_e(t)
                gather_f(t)

        return carry

    lax.fori_loop(0, STEPS, step, 0)

    for n in range(PIECES):
        for j in range(CHUNKS):
            hop_arrived(FINAL + n, j)
            result_ref[n * PIECE : (n + 1) * PIECE, j * CW : (j + 1) * CW] = inbox[FINAL + n, j]

    def drain(k, carry):
        for j in range(CHUNKS):
            hop(k, j).wait_send()
        return carry

    lax.fori_loop(0, STEPS, drain, 0)
    for t in range(4):
        for e in range(EVENTS):
            outgoing(t, e).wait_send()


def per_device(hidden_in, norm_gain, qkv_weight, qkv_bias, out_weight):
    rope, mask = tables()
    vmem = pl.BlockSpec(memory_space=pltpu.VMEM)
    anywhere = pl.BlockSpec(memory_space=pl.ANY)
    dma = pltpu.SemaphoreType.DMA
    result = pl.pallas_call(
        kernel,
        name="sections",
        out_shape=jax.ShapeDtypeStruct((LEN, D), jnp.bfloat16),
        in_specs=[anywhere, vmem, anywhere, vmem, anywhere, vmem, vmem],
        out_specs=vmem,
        scratch_shapes=[
            pltpu.VMEM((2, D, QKV), jnp.bfloat16),
            pltpu.VMEM((2, D, D), jnp.bfloat16),
            pltpu.VMEM((STEPS + PIECES, CHUNKS, PIECE, CW), jnp.bfloat16),
            pltpu.VMEM((STEPS, CHUNKS, PIECE, CW), jnp.bfloat16),
            pltpu.VMEM((PIECE, QKV), jnp.float32),
            pltpu.VMEM((KV_HEADS, LEN, 2 * HEAD_DIM), jnp.bfloat16),
            pltpu.VMEM((KV_HEADS, LEN, 2 * HEAD_DIM), jnp.bfloat16),
            dma((4,)),
            dma((4, EVENTS)),
            dma((4, EVENTS)),
            dma((STEPS, CHUNKS)),
            dma((STEPS + PIECES, CHUNKS)),
        ],
        compiler_params=pltpu.CompilerParams(collective_id=0, has_side_effects=True),
    )(hidden_in, norm_gain, qkv_weight, qkv_bias, out_weight, rope, mask)
    return result[None, None]


def solution(mesh):
    in_specs = (
        P(None, "fsdp", None, None),
        P(None, "section", None),
        P(None, "section", "fsdp", None),
        P(None, "section", None),
        P(None, "section", "fsdp", None),
    )
    out_specs = P("section", "fsdp", None, None)
    return jax.shard_map(
        per_device, mesh=mesh, in_specs=in_specs, out_specs=out_specs, check_vma=False
    )
```

```python
import functools
import math

import jax
import jax.numpy as jnp
import numpy as np
from jax import lax
from jax.experimental import pallas as pl
from jax.experimental.pallas import tpu as pltpu
from jax.sharding import PartitionSpec as P

HEADS = 12
KV_HEADS = 2
HEAD_DIM = 128
GROUP = HEADS // KV_HEADS
LEN = 64
PIECE = 32
PIECES = LEN // PIECE
D = HEADS * HEAD_DIM
QKV = D + 2 * KV_HEADS * HEAD_DIM
SECTIONS = 8
FSDP = 16
ROWS = D // FSDP
HALF = ROWS // 2
MICRO = 8
PASS = MICRO * PIECES
STEPS = 2 * PASS
CHUNKS = 3
CW = D // CHUNKS
FINAL = STEPS
THETA = 1000000.0
EPS = 1.0
SLAB = 80
MESH = pl.DeviceIdType.MESH


def tables():
    frequency = np.exp(np.arange(HEAD_DIM // 2) * (-2.0 * math.log(THETA) / HEAD_DIM))
    angles = np.arange(LEN)[:, None] * frequency[None, :]
    cosine, sine = np.cos(angles), np.sin(angles)
    full_cos = np.concatenate([cosine, cosine], axis=1)
    full_sin = np.concatenate([-sine, sine], axis=1)
    scale = 1.0 / math.sqrt(HEAD_DIM)
    mask = np.where(np.arange(LEN)[:, None] >= np.arange(LEN)[None, :], 0.0, -1e30)
    rope = np.stack([full_cos * scale, full_sin * scale, full_cos, full_sin])
    rope = rope.reshape(4, PIECES, PIECE, HEAD_DIM).swapaxes(0, 1)
    mask = mask.reshape(PIECES, PIECE, LEN)
    return rope.astype(np.float32), mask.astype(np.float32)


def split_two(value):
    high = value.astype(jnp.bfloat16)
    low = (value - high.astype(jnp.float32)).astype(jnp.bfloat16)
    return high, low


def kernel(
    hidden_hbm,
    gain_ref,
    qkv_hbm,
    bias_ref,
    out_hbm,
    rope_ref,
    mask_ref,
    result_ref,
    wq,
    wo,
    inbox,
    outbox,
    acc,
    keys,
    values,
    own_sem,
    gsend,
    grecv,
    hsend,
    hrecv,
):
    s = lax.axis_index("section")
    f = lax.axis_index("fsdp")
    y = lax.div(f, 4)
    low = lax.rem(f, 4)
    x = lax.div(low, 2)
    core = lax.rem(f, 2)
    mirrored = f + 2 - 4 * x
    x_other = low + 2 - 4 * x
    y_next = lax.rem(y + 1, 4) * 4
    y_prev = lax.rem(y + 3, 4) * 4
    y_far = lax.rem(y + 2, 4) * 4
    flip = 1 - 2 * core

    dev_next = y_next + low
    dev_prev = y_prev + low
    dev_x = mirrored
    dev_sib = f + flip

    blocks = (
        f,
        y_prev + low,
        y_next + low,
        mirrored,
        y_far + low,
        y_prev + x_other,
        y_next + x_other,
        y_far + x_other,
    )
    OWN, PREV, NEXT, ACROSS, FAR, XPREV, XNEXT, XFAR = blocks

    tensors = ((wq, 0), (wo, 0), (wq, 1), (wo, 1))
    sources = ((qkv_hbm, 0), (out_hbm, 0), (qkv_hbm, 1), (out_hbm, 1))

    def region(t, block, first=0, count=ROWS):
        ref, layer = tensors[t]
        start = pl.multiple_of(block * ROWS + first, 16)
        return ref.at[layer, pl.ds(start, count), :]

    sends = {
        0: (OWN, 0, ROWS, dev_next),
        1: (OWN, 0, ROWS, dev_prev),
        2: (OWN, 0, ROWS, dev_x),
        3: (PREV, 0, HALF, dev_next),
        4: (NEXT, HALF, HALF, dev_prev),
        5: (ACROSS, 0, SLAB, dev_next),
        6: (ACROSS, 0, SLAB, dev_prev),
        7: (FAR, 0, ROWS, dev_x),
        16: (PREV, SLAB, ROWS - SLAB, dev_x),
        17: (NEXT, SLAB, ROWS - SLAB, dev_x),
    }
    lands = {
        0: (PREV, 0, ROWS),
        1: (NEXT, 0, ROWS),
        2: (ACROSS, 0, ROWS),
        3: (FAR, 0, HALF),
        4: (FAR, HALF, HALF),
        5: (XPREV, 0, SLAB),
        6: (XNEXT, 0, SLAB),
        7: (XFAR, 0, ROWS),
        16: (XPREV, SLAB, ROWS - SLAB),
        17: (XNEXT, SLAB, ROWS - SLAB),
    }
    for n in range(8):
        sends[8 + n] = (blocks[n], 0, ROWS, dev_sib)
        lands[8 + n] = (blocks[n] + flip, 0, ROWS)

    def arrival(e):
        return e if e < 8 else 8 if e < 16 else e - 7

    def outgoing(t, e):
        block, first, count, target = sends[e]
        part = region(t, block, first, count)
        return pltpu.make_async_remote_copy(
            src_ref=part,
            dst_ref=part,
            send_sem=gsend.at[t],
            recv_sem=grecv.at[t, arrival(e)],
            device_id=(s, target),
            device_id_type=MESH,
        )

    def arrived(t, e):
        block, first, count = lands[e]
        part = region(t, block, first, count)
        pltpu.make_async_remote_copy(
            src_ref=part,
            dst_ref=part,
            send_sem=gsend.at[t],
            recv_sem=grecv.at[t, arrival(e)],
            device_id=(s, dev_sib),
            device_id_type=MESH,
        ).wait_recv()

    def own_copy(t):
        ref, layer = sources[t]
        return pltpu.make_async_copy(ref.at[layer, 0], region(t, OWN), own_sem.at[t])

    def gather_a(t):
        own_copy(t).wait()
        for e in (0, 1, 2, 8):
            outgoing(t, e).start()

    def gather_b(t):
        for e, then in ((0, (3, 16, 9)), (1, (4, 17, 10))):
            arrived(t, e)
            for n in then:
                outgoing(t, n).start()

    def gather_c(t):
        arrived(t, 2)
        for n in (5, 6, 11):
            outgoing(t, n).start()

    def gather_d(t):
        arrived(t, 3)
        arrived(t, 4)
        for n in (7, 12):
            outgoing(t, n).start()

    def gather_e(t):
        for e, then in ((5, None), (16, 13), (6, None), (17, 14), (7, 15)):
            arrived(t, e)
            if then is not None:
                outgoing(t, then).start()

    def gather_f(t):
        whole = region(t, 0, 0, 8 * ROWS)
        pltpu.make_async_remote_copy(
            src_ref=whole,
            dst_ref=whole,
            send_sem=gsend.at[t],
            recv_sem=grecv.at[t, 8],
            device_id=(s, dev_sib),
            device_id_type=MESH,
        ).wait_recv()

    def gather_sent(t):
        whole = region(t, 0, 0, sum(count for _, _, count, _ in sends.values()))
        pltpu.make_async_remote_copy(
            src_ref=whole,
            dst_ref=whole,
            send_sem=gsend.at[t],
            recv_sem=grecv.at[t, 8],
            device_id=(s, dev_sib),
            device_id_type=MESH,
        ).wait_send()

    def entering(k, j):
        return pltpu.make_async_copy(
            hidden_hbm.at[k // PIECES, 0, pl.ds(k % PIECES * PIECE, PIECE), pl.ds(j * CW, CW)],
            inbox.at[k, j],
            hrecv.at[k, j],
        )

    for t in range(4):
        own_copy(t).start()

    @pl.when(s == 0)
    def _():
        for k in range(PASS):
            for j in range(CHUNKS):
                entering(k, j).start()

    crossing_in = (s == 4) | (s == 0)
    crossing_out = (s == 3) | (s == SECTIONS - 1)
    before = (lax.rem(s + SECTIONS - 1, SECTIONS), jnp.where(crossing_in, mirrored, f))
    after_f = jnp.where(crossing_out, mirrored, f)
    barrier = pltpu.get_barrier_semaphore()
    greeted = [(s, dev_next), (s, dev_prev), (s, dev_x), (s, dev_sib), before]
    greeted.append((SECTIONS - 1, mirrored))
    for device in greeted:
        pl.semaphore_signal(barrier, inc=1, device_id=device, device_id_type=MESH)
    pl.semaphore_wait(barrier, 5 + jnp.where(s == SECTIONS - 1, SECTIONS, 0))

    gather_a(0)
    gather_a(1)
    keys[...] = jnp.zeros_like(keys)
    values[...] = jnp.ones_like(values)
    gather_b(0)
    gather_b(1)
    gather_c(0)
    gather_c(1)
    gather_d(0)
    gather_d(1)
    gather_e(0)
    gather_f(0)

    gather_e(1)
    gather_f(1)
    gather_a(2)
    gather_a(3)

    def hop(k, j):
        last = s == SECTIONS - 1
        second = k >= PASS
        owner = lax.div(k, PIECES) - MICRO
        to_section = jnp.where(last, jnp.where(second, owner, 0), s + 1)
        slot = jnp.where(last, jnp.where(second, FINAL + lax.rem(k, PIECES), k + PASS), k)
        return pltpu.make_async_remote_copy(
            src_ref=outbox.at[k, j],
            dst_ref=inbox.at[slot, j],
            send_sem=hsend.at[0],
            recv_sem=hrecv.at[slot, j],
            device_id=(to_section, after_f),
            device_id_type=MESH,
        )

    def hop_arrived(slot, j):
        pltpu.make_async_remote_copy(
            src_ref=inbox.at[slot, j],
            dst_ref=inbox.at[slot, j],
            send_sem=hsend.at[0],
            recv_sem=hrecv.at[slot, j],
            device_id=(s, dev_sib),
            device_id_type=MESH,
        ).wait_recv()

    def layer(k):
        c = lax.div(k, PASS)
        piece = lax.rem(k, PIECES)
        squares = jnp.zeros((PIECE, 128), jnp.float32)
        for j in range(CHUNKS):
            hop_arrived(k, j)
            wide = inbox[k, j].astype(jnp.float32)
            for p in range(CW // 128):
                part = wide[:, p * 128 : (p + 1) * 128]
                squares = squares + part * part
            scaled = (wide * gain_ref[c, :, j * CW : (j + 1) * CW]).astype(jnp.bfloat16)
            for n in (3, 0, 1, 2):
                cols = slice(n * 512, (n + 1) * 512)
                product = jnp.dot(
                    scaled,
                    wq[c, j * CW : (j + 1) * CW, cols],
                    preferred_element_type=jnp.float32,
                )
                if j > 0:
                    product = product + acc[:, cols]
                acc[:, cols] = product
        inv = lax.rsqrt(jnp.sum(squares, axis=1, keepdims=True) * (1.0 / D) + EPS)

        def projected(col, width=HEAD_DIM):
            cols = slice(col, col + width)
            return acc[:, cols] * inv + bias_ref[c, :, cols]

        def rotated(value, table):
            turned = pltpu.roll(value, HEAD_DIM // 2, 1)
            return value * rope_ref[piece, table] + turned * rope_ref[piece, table + 1]

        rows = pl.ds(pl.multiple_of(piece * PIECE, PIECE), PIECE)
        for g in range(KV_HEADS):
            key_high, key_low = split_two(rotated(projected(D + g * HEAD_DIM), 2))
            keys[g, rows, :HEAD_DIM] = key_high
            keys[g, rows, HEAD_DIM:] = key_low
            value_rows = projected(D + (KV_HEADS + g) * HEAD_DIM)
            values[g, rows, :HEAD_DIM] = value_rows.astype(jnp.bfloat16)
        contract = (((1,), (1,)), ((), ()))
        mask = jnp.concatenate([mask_ref[piece]] * GROUP, axis=0)
        scores = []
        for g in range(KV_HEADS):
            heads = [
                split_two(rotated(projected((g * GROUP + h) * HEAD_DIM), 0))
                for h in range(GROUP)
            ]
            query_high = jnp.concatenate([h[0] for h in heads], axis=0)
            query_low = jnp.concatenate([h[1] for h in heads], axis=0)
            key_high = keys[g, :, :HEAD_DIM]
            key_low = keys[g, :, HEAD_DIM:]
            scores.append(
                lax.dot_general(
                    jnp.concatenate([query_high, query_low, query_high], axis=1),
                    jnp.concatenate([key_high, key_high, key_low], axis=1),
                    contract,
                    preferred_element_type=jnp.float32,
                )
            )
        weights = []
        for g in range(KV_HEADS):
            masked = scores[g] + mask
            shifted = masked - jnp.max(masked, axis=1, keepdims=True)
            weights.append(jnp.exp(shifted).astype(jnp.bfloat16))
        mixed = [
            jnp.dot(weights[g], values[g], preferred_element_type=jnp.float32)
            for g in range(KV_HEADS)
        ]
        contexts = []
        for g in range(KV_HEADS):
            context = (mixed[g][:, :HEAD_DIM] / mixed[g][:, HEAD_DIM:]).astype(jnp.bfloat16)
            contexts.append(
                jnp.concatenate(
                    [context[h * PIECE : (h + 1) * PIECE] for h in range(GROUP)], axis=1
                )
            )

        updates = [None] * CHUNKS
        half = GROUP * HEAD_DIM

        def finish(j):
            total = inbox[k, j].astype(jnp.float32) + updates[j]
            outbox[k, j] = total.astype(jnp.bfloat16)
            hop(k, j).start()

        for j in range(CHUNKS):
            for g in range(KV_HEADS):
                product = jnp.dot(
                    contexts[g],
                    wo[c, g * half : (g + 1) * half, j * CW : (j + 1) * CW],
                    preferred_element_type=jnp.float32,
                )
                updates[j] = product if g == 0 else updates[j] + product
            if j > 0:
                finish(j - 1)
        finish(CHUNKS - 1)

    def step(k, carry):
        layer(k)

        @pl.when(k == 4)
        def _():
            gather_b(2)

        @pl.when(k == 7)
        def _():
            gather_b(3)
            gather_c(2)
            gather_c(3)

        @pl.when(k == 9)
        def _():
            gather_d(2)
            gather_d(3)

        @pl.when(k == 15)
        def _():
            for t in (2, 3):
                gather_e(t)
                gather_f(t)

        return carry

    lax.fori_loop(0, STEPS, step, 0)

    pltpu.make_async_remote_copy(
        src_ref=outbox,
        dst_ref=outbox,
        send_sem=hsend.at[0],
        recv_sem=hrecv.at[0, 0],
        device_id=(s, dev_sib),
        device_id_type=MESH,
    ).wait_send()
    for t in range(4):
        gather_sent(t)

    for n in range(PIECES):
        for j in range(CHUNKS):
            hop_arrived(FINAL + n, j)
            result_ref[n * PIECE : (n + 1) * PIECE, j * CW : (j + 1) * CW] = inbox[FINAL + n, j]


def per_device(hidden_in, norm_gain, qkv_weight, qkv_bias, out_weight):
    rope, mask = tables()
    vmem = pl.BlockSpec(memory_space=pltpu.VMEM)
    anywhere = pl.BlockSpec(memory_space=pl.ANY)
    dma = pltpu.SemaphoreType.DMA
    result = pl.pallas_call(
        kernel,
        name="sections",
        out_shape=jax.ShapeDtypeStruct((LEN, D), jnp.bfloat16),
        in_specs=[anywhere, vmem, anywhere, vmem, anywhere, vmem, vmem],
        out_specs=vmem,
        scratch_shapes=[
            pltpu.VMEM((2, D, QKV), jnp.bfloat16),
            pltpu.VMEM((2, D, D), jnp.bfloat16),
            pltpu.VMEM((STEPS + PIECES, CHUNKS, PIECE, CW), jnp.bfloat16),
            pltpu.VMEM((STEPS, CHUNKS, PIECE, CW), jnp.bfloat16),
            pltpu.VMEM((PIECE, QKV), jnp.float32),
            pltpu.VMEM((KV_HEADS, LEN, 2 * HEAD_DIM), jnp.bfloat16),
            pltpu.VMEM((KV_HEADS, LEN, 2 * HEAD_DIM), jnp.bfloat16),
            dma((4,)),
            dma((4,)),
            dma((4, 11)),
            dma((1,)),
            dma((STEPS + PIECES, CHUNKS)),
        ],
        compiler_params=pltpu.CompilerParams(collective_id=0, has_side_effects=True),
    )(hidden_in, norm_gain, qkv_weight, qkv_bias, out_weight, rope, mask)
    return result[None, None]


def solution(mesh):
    in_specs = (
        P(None, "fsdp", None, None),
        P(None, "section", None),
        P(None, "section", "fsdp", None),
        P(None, "section", None),
        P(None, "section", "fsdp", None),
    )
    out_specs = P("section", "fsdp", None, None)
    return jax.shard_map(
        per_device, mesh=mesh, in_specs=in_specs, out_specs=out_specs, check_vma=False
    )
```

```python
import functools
import math

import jax
import jax.numpy as jnp
import numpy as np
from jax import lax
from jax.experimental import pallas as pl
from jax.experimental.pallas import tpu as pltpu
from jax.sharding import PartitionSpec as P

HEADS = 12
KV_HEADS = 2
HEAD_DIM = 128
GROUP = HEADS // KV_HEADS
LEN = 64
PIECE = 32
PIECES = LEN // PIECE
D = HEADS * HEAD_DIM
QKV = D + 2 * KV_HEADS * HEAD_DIM
SECTIONS = 8
FSDP = 16
ROWS = D // FSDP
HALF = ROWS // 2
MICRO = 8
PASS = MICRO * PIECES
STEPS = 2 * PASS
CHUNKS = 3
CW = D // CHUNKS
FINAL = STEPS
THETA = 1000000.0
EPS = 1.0
SLAB = 80
MESH = pl.DeviceIdType.MESH


def tables():
    frequency = np.exp(np.arange(HEAD_DIM // 2) * (-2.0 * math.log(THETA) / HEAD_DIM))
    angles = np.arange(LEN)[:, None] * frequency[None, :]
    cosine, sine = np.cos(angles), np.sin(angles)
    full_cos = np.concatenate([cosine, cosine], axis=1)
    full_sin = np.concatenate([-sine, sine], axis=1)
    scale = 1.0 / math.sqrt(HEAD_DIM)
    mask = np.where(np.arange(LEN)[:, None] >= np.arange(LEN)[None, :], 0.0, -1e30)
    rope = np.stack([full_cos * scale, full_sin * scale, full_cos, full_sin])
    rope = rope.reshape(4, PIECES, PIECE, HEAD_DIM).swapaxes(0, 1)
    mask = mask.reshape(PIECES, PIECE, LEN)
    return rope.astype(np.float32), mask.astype(np.float32)


def split_two(value):
    high = value.astype(jnp.bfloat16)
    low = (value - high.astype(jnp.float32)).astype(jnp.bfloat16)
    return high, low


def kernel(
    hidden_hbm,
    gain_ref,
    qkv_hbm,
    bias_ref,
    out_hbm,
    rope_ref,
    mask_ref,
    result_ref,
    wq,
    wo,
    inbox,
    outbox,
    acc,
    keys,
    values,
    own_sem,
    gsend,
    grecv,
    hsend,
    hrecv,
):
    s = lax.axis_index("section")
    f = lax.axis_index("fsdp")
    y = lax.div(f, 4)
    low = lax.rem(f, 4)
    x = lax.div(low, 2)
    core = lax.rem(f, 2)
    mirrored = f + 2 - 4 * x
    x_other = low + 2 - 4 * x
    y_next = lax.rem(y + 1, 4) * 4
    y_prev = lax.rem(y + 3, 4) * 4
    y_far = lax.rem(y + 2, 4) * 4
    flip = 1 - 2 * core

    dev_next = y_next + low
    dev_prev = y_prev + low
    dev_x = mirrored
    dev_sib = f + flip

    blocks = (
        f,
        y_prev + low,
        y_next + low,
        mirrored,
        y_far + low,
        y_prev + x_other,
        y_next + x_other,
        y_far + x_other,
    )
    OWN, PREV, NEXT, ACROSS, FAR, XPREV, XNEXT, XFAR = blocks

    tensors = ((wq, 0), (wo, 0), (wq, 1), (wo, 1))
    sources = ((qkv_hbm, 0), (out_hbm, 0), (qkv_hbm, 1), (out_hbm, 1))

    def region(t, block, first=0, count=ROWS):
        ref, layer = tensors[t]
        start = pl.multiple_of(block * ROWS + first, 16)
        return ref.at[layer, pl.ds(start, count), :]

    sends = {
        0: (OWN, 0, ROWS, dev_next),
        1: (OWN, 0, ROWS, dev_prev),
        2: (OWN, 0, ROWS, dev_x),
        3: (PREV, 0, HALF, dev_next),
        4: (NEXT, HALF, HALF, dev_prev),
        5: (ACROSS, 0, SLAB, dev_next),
        6: (ACROSS, 0, SLAB, dev_prev),
        7: (FAR, 0, ROWS, dev_x),
        16: (PREV, SLAB, ROWS - SLAB, dev_x),
        17: (NEXT, SLAB, ROWS - SLAB, dev_x),
    }
    lands = {
        0: (PREV, 0, ROWS),
        1: (NEXT, 0, ROWS),
        2: (ACROSS, 0, ROWS),
        3: (FAR, 0, ROWS),
        5: (XPREV, 0, ROWS),
        6: (XNEXT, 0, ROWS),
        7: (XFAR, 0, ROWS),
    }
    for n in range(8):
        sends[8 + n] = (blocks[n], 0, ROWS, dev_sib)
        lands[8 + n] = (blocks[n] + flip, 0, ROWS)

    def arrival(e):
        return {4: 3, 5: 4, 16: 4, 6: 5, 17: 5, 7: 6}.get(e, e if e < 4 else 7)

    def outgoing(t, e):
        block, first, count, target = sends[e]
        part = region(t, block, first, count)
        return pltpu.make_async_remote_copy(
            src_ref=part,
            dst_ref=part,
            send_sem=gsend.at[t],
            recv_sem=grecv.at[t, arrival(e)],
            device_id=(s, target),
            device_id_type=MESH,
        )

    def arrived(t, e):
        block, first, count = lands[e]
        part = region(t, block, first, count)
        pltpu.make_async_remote_copy(
            src_ref=part,
            dst_ref=part,
            send_sem=gsend.at[t],
            recv_sem=grecv.at[t, arrival(e)],
            device_id=(s, dev_sib),
            device_id_type=MESH,
        ).wait_recv()

    def own_copy(t):
        ref, layer = sources[t]
        return pltpu.make_async_copy(ref.at[layer, 0], region(t, OWN), own_sem.at[t])

    def gather_a(t):
        own_copy(t).wait()
        for e in (0, 1, 2, 8):
            outgoing(t, e).start()

    def gather_b(t):
        for e, then in ((0, (3, 16, 9)), (1, (4, 17, 10))):
            arrived(t, e)
            for n in then:
                outgoing(t, n).start()

    def gather_c(t):
        arrived(t, 2)
        for n in (5, 6, 11):
            outgoing(t, n).start()

    def gather_d(t):
        arrived(t, 3)
        for n in (7, 12):
            outgoing(t, n).start()

    def gather_e(t):
        for e, then in ((5, 13), (6, 14), (7, 15)):
            arrived(t, e)
            outgoing(t, then).start()

    def gather_f(t):
        whole = region(t, 0, 0, 8 * ROWS)
        pltpu.make_async_remote_copy(
            src_ref=whole,
            dst_ref=whole,
            send_sem=gsend.at[t],
            recv_sem=grecv.at[t, arrival(8)],
            device_id=(s, dev_sib),
            device_id_type=MESH,
        ).wait_recv()

    def gather_sent(t):
        whole = region(t, 0, 0, sum(count for _, _, count, _ in sends.values()))
        pltpu.make_async_remote_copy(
            src_ref=whole,
            dst_ref=whole,
            send_sem=gsend.at[t],
            recv_sem=grecv.at[t, arrival(8)],
            device_id=(s, dev_sib),
            device_id_type=MESH,
        ).wait_send()

    def arrival_row(slot):
        return slot % PASS

    def entering(k, j):
        return pltpu.make_async_copy(
            hidden_hbm.at[k // PIECES, 0, pl.ds(k % PIECES * PIECE, PIECE), pl.ds(j * CW, CW)],
            inbox.at[k, j],
            hrecv.at[arrival_row(k), j],
        )

    for t in range(4):
        own_copy(t).start()

    @pl.when(s == 0)
    def _():
        for k in range(PASS):
            for j in range(CHUNKS):
                entering(k, j).start()

    crossing_in = (s == 4) | (s == 0)
    crossing_out = (s == 3) | (s == SECTIONS - 1)
    before = (lax.rem(s + SECTIONS - 1, SECTIONS), jnp.where(crossing_in, mirrored, f))
    after_f = jnp.where(crossing_out, mirrored, f)
    barrier = pltpu.get_barrier_semaphore()
    greeted = [(s, dev_next), (s, dev_prev), (s, dev_x), (s, dev_sib), before]
    greeted.append((SECTIONS - 1, mirrored))
    for device in greeted:
        pl.semaphore_signal(barrier, inc=1, device_id=device, device_id_type=MESH)
    pl.semaphore_wait(barrier, 5 + jnp.where(s == SECTIONS - 1, SECTIONS, 0))

    gather_a(0)
    gather_a(1)
    keys[...] = jnp.zeros_like(keys)
    values[...] = jnp.ones_like(values)
    gather_b(0)
    gather_b(1)
    gather_c(0)
    gather_c(1)
    gather_d(0)
    gather_d(1)
    gather_e(0)
    gather_f(0)

    gather_e(1)
    gather_f(1)
    gather_a(2)
    gather_a(3)

    def hop(k, j):
        last = s == SECTIONS - 1
        second = k >= PASS
        owner = lax.div(k, PIECES) - MICRO
        to_section = jnp.where(last, jnp.where(second, owner, 0), s + 1)
        slot = jnp.where(last, jnp.where(second, FINAL + lax.rem(k, PIECES), k + PASS), k)
        done = last & second
        row = jnp.where(done, PASS, lax.rem(k, PASS))
        column = jnp.where(done, 0, j)
        return pltpu.make_async_remote_copy(
            src_ref=outbox.at[k, j],
            dst_ref=inbox.at[slot, j],
            send_sem=hsend.at[0],
            recv_sem=hrecv.at[row, column],
            device_id=(to_section, after_f),
            device_id_type=MESH,
        )

    def hop_arrived(slot, j):
        pltpu.make_async_remote_copy(
            src_ref=inbox.at[slot, j],
            dst_ref=inbox.at[slot, j],
            send_sem=hsend.at[0],
            recv_sem=hrecv.at[lax.rem(slot, PASS), j],
            device_id=(s, dev_sib),
            device_id_type=MESH,
        ).wait_recv()

    def layer(k):
        c = lax.div(k, PASS)
        piece = lax.rem(k, PIECES)
        squares = jnp.zeros((PIECE, 128), jnp.float32)
        for j in range(CHUNKS):
            hop_arrived(k, j)
            wide = inbox[k, j].astype(jnp.float32)
            for p in range(CW // 128):
                part = wide[:, p * 128 : (p + 1) * 128]
                squares = squares + part * part
            scaled = (wide * gain_ref[c, :, j * CW : (j + 1) * CW]).astype(jnp.bfloat16)
            for n in (3, 0, 1, 2):
                cols = slice(n * 512, (n + 1) * 512)
                product = jnp.dot(
                    scaled,
                    wq[c, j * CW : (j + 1) * CW, cols],
                    preferred_element_type=jnp.float32,
                )
                if j > 0:
                    product = product + acc[:, cols]
                acc[:, cols] = product
        inv = lax.rsqrt(jnp.sum(squares, axis=1, keepdims=True) * (1.0 / D) + EPS)

        def projected(col, width=HEAD_DIM):
            cols = slice(col, col + width)
            return acc[:, cols] * inv + bias_ref[c, :, cols]

        def rotated(value, table):
            turned = pltpu.roll(value, HEAD_DIM // 2, 1)
            return value * rope_ref[piece, table] + turned * rope_ref[piece, table + 1]

        rows = pl.ds(pl.multiple_of(piece * PIECE, PIECE), PIECE)
        for g in range(KV_HEADS):
            key_high, key_low = split_two(rotated(projected(D + g * HEAD_DIM), 2))
            keys[g, rows, :HEAD_DIM] = key_high
            keys[g, rows, HEAD_DIM:] = key_low
            value_rows = projected(D + (KV_HEADS + g) * HEAD_DIM)
            values[g, rows, :HEAD_DIM] = value_rows.astype(jnp.bfloat16)
        contract = (((1,), (1,)), ((), ()))
        mask = jnp.concatenate([mask_ref[piece]] * GROUP, axis=0)
        scores = []
        for g in range(KV_HEADS):
            heads = [
                split_two(rotated(projected((g * GROUP + h) * HEAD_DIM), 0))
                for h in range(GROUP)
            ]
            query_high = jnp.concatenate([h[0] for h in heads], axis=0)
            query_low = jnp.concatenate([h[1] for h in heads], axis=0)
            key_high = keys[g, :, :HEAD_DIM]
            key_low = keys[g, :, HEAD_DIM:]
            scores.append(
                lax.dot_general(
                    jnp.concatenate([query_high, query_low, query_high], axis=1),
                    jnp.concatenate([key_high, key_high, key_low], axis=1),
                    contract,
                    preferred_element_type=jnp.float32,
                )
            )
        weights = []
        for g in range(KV_HEADS):
            masked = scores[g] + mask
            shifted = masked - jnp.max(masked, axis=1, keepdims=True)
            weights.append(jnp.exp(shifted).astype(jnp.bfloat16))
        mixed = [
            jnp.dot(weights[g], values[g], preferred_element_type=jnp.float32)
            for g in range(KV_HEADS)
        ]
        contexts = []
        for g in range(KV_HEADS):
            context = (mixed[g][:, :HEAD_DIM] / mixed[g][:, HEAD_DIM:]).astype(jnp.bfloat16)
            contexts.append(
                jnp.concatenate(
                    [context[h * PIECE : (h + 1) * PIECE] for h in range(GROUP)], axis=1
                )
            )

        updates = [None] * CHUNKS
        half = GROUP * HEAD_DIM

        def finish(j):
            total = inbox[k, j].astype(jnp.float32) + updates[j]
            outbox[k, j] = total.astype(jnp.bfloat16)
            hop(k, j).start()

        for j in range(CHUNKS):
            for g in range(KV_HEADS):
                product = jnp.dot(
                    contexts[g],
                    wo[c, g * half : (g + 1) * half, j * CW : (j + 1) * CW],
                    preferred_element_type=jnp.float32,
                )
                updates[j] = product if g == 0 else updates[j] + product
            if j > 0:
                finish(j - 1)
        finish(CHUNKS - 1)

    def step(k, carry):
        layer(k)

        @pl.when(k == 4)
        def _():
            gather_b(2)

        @pl.when(k == 7)
        def _():
            gather_b(3)
            gather_c(2)
            gather_c(3)

        @pl.when(k == 9)
        def _():
            gather_d(2)
            gather_d(3)

        @pl.when(k == 15)
        def _():
            for t in (2, 3):
                gather_e(t)
                gather_f(t)

        return carry

    lax.fori_loop(0, STEPS, step, 0)

    pltpu.make_async_remote_copy(
        src_ref=outbox,
        dst_ref=outbox,
        send_sem=hsend.at[0],
        recv_sem=hrecv.at[0, 0],
        device_id=(s, dev_sib),
        device_id_type=MESH,
    ).wait_send()
    for t in range(4):
        gather_sent(t)

    finished = inbox.at[pl.ds(FINAL, PIECES)]
    pltpu.make_async_remote_copy(
        src_ref=finished,
        dst_ref=finished,
        send_sem=hsend.at[0],
        recv_sem=hrecv.at[PASS, 0],
        device_id=(s, dev_sib),
        device_id_type=MESH,
    ).wait_recv()
    for n in range(PIECES):
        for j in range(CHUNKS):
            result_ref[n * PIECE : (n + 1) * PIECE, j * CW : (j + 1) * CW] = inbox[FINAL + n, j]


def per_device(hidden_in, norm_gain, qkv_weight, qkv_bias, out_weight):
    rope, mask = tables()
    vmem = pl.BlockSpec(memory_space=pltpu.VMEM)
    anywhere = pl.BlockSpec(memory_space=pl.ANY)
    dma = pltpu.SemaphoreType.DMA
    result = pl.pallas_call(
        kernel,
        name="sections",
        out_shape=jax.ShapeDtypeStruct((LEN, D), jnp.bfloat16),
        in_specs=[anywhere, vmem, anywhere, vmem, anywhere, vmem, vmem],
        out_specs=vmem,
        scratch_shapes=[
            pltpu.VMEM((2, D, QKV), jnp.bfloat16),
            pltpu.VMEM((2, D, D), jnp.bfloat16),
            pltpu.VMEM((STEPS + PIECES, CHUNKS, PIECE, CW), jnp.bfloat16),
            pltpu.VMEM((STEPS, CHUNKS, PIECE, CW), jnp.bfloat16),
            pltpu.VMEM((PIECE, QKV), jnp.float32),
            pltpu.VMEM((KV_HEADS, LEN, 2 * HEAD_DIM), jnp.bfloat16),
            pltpu.VMEM((KV_HEADS, LEN, 2 * HEAD_DIM), jnp.bfloat16),
            dma((4,)),
            dma((4,)),
            dma((4, 8)),
            dma((1,)),
            dma((PASS + 1, CHUNKS)),
        ],
        compiler_params=pltpu.CompilerParams(collective_id=0, has_side_effects=True),
    )(hidden_in, norm_gain, qkv_weight, qkv_bias, out_weight, rope, mask)
    return result[None, None]


def solution(mesh):
    in_specs = (
        P(None, "fsdp", None, None),
        P(None, "section", None),
        P(None, "section", "fsdp", None),
        P(None, "section", None),
        P(None, "section", "fsdp", None),
    )
    out_specs = P("section", "fsdp", None, None)
    return jax.shard_map(
        per_device, mesh=mesh, in_specs=in_specs, out_specs=out_specs, check_vma=False
    )
```

```python
import functools
import math

import jax
import jax.numpy as jnp
import numpy as np
from jax import lax
from jax.experimental import pallas as pl
from jax.experimental.pallas import tpu as pltpu
from jax.sharding import PartitionSpec as P

HEADS = 12
KV_HEADS = 2
HEAD_DIM = 128
GROUP = HEADS // KV_HEADS
LEN = 64
PIECE = 32
PIECES = LEN // PIECE
D = HEADS * HEAD_DIM
QKV = D + 2 * KV_HEADS * HEAD_DIM
SECTIONS = 8
FSDP = 16
ROWS = D // FSDP
HALF = ROWS // 2
MICRO = 8
PASS = MICRO * PIECES
STEPS = 2 * PASS
CHUNKS = 3
CW = D // CHUNKS
FINAL = STEPS
THETA = 1000000.0
EPS = 1.0
SLAB = 80
MESH = pl.DeviceIdType.MESH


def tables():
    frequency = np.exp(np.arange(HEAD_DIM // 2) * (-2.0 * math.log(THETA) / HEAD_DIM))
    angles = np.arange(LEN)[:, None] * frequency[None, :]
    cosine, sine = np.cos(angles), np.sin(angles)
    full_cos = np.concatenate([cosine, cosine], axis=1)
    full_sin = np.concatenate([-sine, sine], axis=1)
    scale = 1.0 / math.sqrt(HEAD_DIM)
    mask = np.where(np.arange(LEN)[:, None] >= np.arange(LEN)[None, :], 0.0, -1e30)
    rope = np.stack([full_cos * scale, full_sin * scale, full_cos, full_sin])
    rope = rope.reshape(4, PIECES, PIECE, HEAD_DIM).swapaxes(0, 1)
    mask = mask.reshape(PIECES, PIECE, LEN)
    return rope.astype(np.float32), mask.astype(np.float32)


def split_two(value):
    high = value.astype(jnp.bfloat16)
    low = (value - high.astype(jnp.float32)).astype(jnp.bfloat16)
    return high, low


def kernel(
    hidden_hbm,
    gain_ref,
    qkv_hbm,
    bias_ref,
    out_hbm,
    rope_ref,
    mask_ref,
    result_ref,
    wq,
    wo,
    inbox,
    outbox,
    acc,
    keys,
    values,
    own_sem,
    gsend,
    grecv,
    hsend,
    hrecv,
):
    s = lax.axis_index("section")
    f = lax.axis_index("fsdp")
    y = lax.div(f, 4)
    low = lax.rem(f, 4)
    x = lax.div(low, 2)
    core = lax.rem(f, 2)
    mirrored = f + 2 - 4 * x
    x_other = low + 2 - 4 * x
    y_next = lax.rem(y + 1, 4) * 4
    y_prev = lax.rem(y + 3, 4) * 4
    y_far = lax.rem(y + 2, 4) * 4
    flip = 1 - 2 * core

    dev_next = y_next + low
    dev_prev = y_prev + low
    dev_x = mirrored
    dev_sib = f + flip

    blocks = (
        f,
        y_prev + low,
        y_next + low,
        mirrored,
        y_far + low,
        y_prev + x_other,
        y_next + x_other,
        y_far + x_other,
    )
    OWN, PREV, NEXT, ACROSS, FAR, XPREV, XNEXT, XFAR = blocks

    tensors = ((wq, 0), (wo, 0), (wq, 1), (wo, 1))
    sources = ((qkv_hbm, 0), (out_hbm, 0), (qkv_hbm, 1), (out_hbm, 1))

    def region(t, block, first=0, count=ROWS):
        ref, layer = tensors[t]
        start = pl.multiple_of(block * ROWS + first, 16)
        return ref.at[layer, pl.ds(start, count), :]

    sends = {
        0: (OWN, 0, ROWS, dev_next),
        1: (OWN, 0, ROWS, dev_prev),
        2: (OWN, 0, ROWS, dev_x),
        3: (PREV, 0, HALF, dev_next),
        4: (NEXT, HALF, HALF, dev_prev),
        5: (ACROSS, 0, SLAB, dev_next),
        6: (ACROSS, 0, SLAB, dev_prev),
        7: (FAR, 0, ROWS, dev_x),
        16: (PREV, SLAB, ROWS - SLAB, dev_x),
        17: (NEXT, SLAB, ROWS - SLAB, dev_x),
    }
    lands = {
        0: (PREV, 0, ROWS),
        1: (NEXT, 0, ROWS),
        2: (ACROSS, 0, ROWS),
        3: (FAR, 0, ROWS),
        5: (XPREV, 0, ROWS),
        6: (XNEXT, 0, ROWS),
        7: (XFAR, 0, ROWS),
    }
    for n in range(8):
        sends[8 + n] = (blocks[n], 0, ROWS, dev_sib)
        lands[8 + n] = (blocks[n] + flip, 0, ROWS)

    def arrival(e):
        return {4: 3, 5: 4, 16: 4, 6: 5, 17: 5, 7: 6}.get(e, e if e < 4 else 7)

    def outgoing(t, e):
        block, first, count, target = sends[e]
        part = region(t, block, first, count)
        return pltpu.make_async_remote_copy(
            src_ref=part,
            dst_ref=part,
            send_sem=gsend.at[t],
            recv_sem=grecv.at[t, arrival(e)],
            device_id=(s, target),
            device_id_type=MESH,
        )

    def arrived(t, e):
        block, first, count = lands[e]
        part = region(t, block, first, count)
        pltpu.make_async_remote_copy(
            src_ref=part,
            dst_ref=part,
            send_sem=gsend.at[t],
            recv_sem=grecv.at[t, arrival(e)],
            device_id=(s, dev_sib),
            device_id_type=MESH,
        ).wait_recv()

    def own_copy(t):
        ref, layer = sources[t]
        return pltpu.make_async_copy(ref.at[layer, 0], region(t, OWN), own_sem.at[t])

    def gather_a(t):
        own_copy(t).wait()
        for e in (0, 1, 2, 8):
            outgoing(t, e).start()

    def gather_b(t):
        for e, then in ((0, (3, 16, 9)), (1, (4, 17, 10))):
            arrived(t, e)
            for n in then:
                outgoing(t, n).start()

    def gather_c(t):
        arrived(t, 2)
        for n in (5, 6, 11):
            outgoing(t, n).start()

    def gather_d(t):
        arrived(t, 3)
        for n in (7, 12):
            outgoing(t, n).start()

    def gather_e(t):
        for e, then in ((5, 13), (6, 14), (7, 15)):
            arrived(t, e)
            outgoing(t, then).start()

    def gather_f(t):
        whole = region(t, 0, 0, 8 * ROWS)
        pltpu.make_async_remote_copy(
            src_ref=whole,
            dst_ref=whole,
            send_sem=gsend.at[t],
            recv_sem=grecv.at[t, arrival(8)],
            device_id=(s, dev_sib),
            device_id_type=MESH,
        ).wait_recv()

    def gather_sent(t):
        whole = region(t, 0, 0, sum(count for _, _, count, _ in sends.values()))
        pltpu.make_async_remote_copy(
            src_ref=whole,
            dst_ref=whole,
            send_sem=gsend.at[t],
            recv_sem=grecv.at[t, arrival(8)],
            device_id=(s, dev_sib),
            device_id_type=MESH,
        ).wait_send()

    def arrival_row(slot):
        return slot % PASS

    def entering(k, j):
        return pltpu.make_async_copy(
            hidden_hbm.at[k // PIECES, 0, pl.ds(k % PIECES * PIECE, PIECE), pl.ds(j * CW, CW)],
            inbox.at[k, j],
            hrecv.at[arrival_row(k), j],
        )

    for t in range(4):
        own_copy(t).start()

    crossing_in = (s == 4) | (s == 0)
    crossing_out = (s == 3) | (s == SECTIONS - 1)
    before = (lax.rem(s + SECTIONS - 1, SECTIONS), jnp.where(crossing_in, mirrored, f))
    after_f = jnp.where(crossing_out, mirrored, f)
    barrier = pltpu.get_barrier_semaphore()
    greeted = [(s, dev_next), (s, dev_prev), (s, dev_x), (s, dev_sib), before]
    greeted.append((SECTIONS - 1, mirrored))
    for device in greeted:
        pl.semaphore_signal(barrier, inc=1, device_id=device, device_id_type=MESH)
    pl.semaphore_wait(barrier, 5 + jnp.where(s == SECTIONS - 1, SECTIONS, 0))

    gather_a(0)
    gather_a(1)

    @pl.when(s == 0)
    def _():
        for k in range(PASS):
            for j in range(CHUNKS):
                entering(k, j).start()

    keys[...] = jnp.zeros_like(keys)
    values[...] = jnp.ones_like(values)
    gather_b(0)
    gather_b(1)
    gather_c(0)
    gather_c(1)
    gather_d(0)
    gather_d(1)
    gather_e(0)
    gather_f(0)

    gather_e(1)
    gather_f(1)
    gather_a(2)
    gather_a(3)

    def hop(k, j):
        last = s == SECTIONS - 1
        second = k >= PASS
        owner = lax.div(k, PIECES) - MICRO
        to_section = jnp.where(last, jnp.where(second, owner, 0), s + 1)
        slot = jnp.where(last, jnp.where(second, FINAL + lax.rem(k, PIECES), k + PASS), k)
        done = last & second
        row = jnp.where(done, PASS, lax.rem(k, PASS))
        column = jnp.where(done, 0, j)
        return pltpu.make_async_remote_copy(
            src_ref=outbox.at[k, j],
            dst_ref=inbox.at[slot, j],
            send_sem=hsend.at[0],
            recv_sem=hrecv.at[row, column],
            device_id=(to_section, after_f),
            device_id_type=MESH,
        )

    def hop_arrived(slot, j):
        pltpu.make_async_remote_copy(
            src_ref=inbox.at[slot, j],
            dst_ref=inbox.at[slot, j],
            send_sem=hsend.at[0],
            recv_sem=hrecv.at[lax.rem(slot, PASS), j],
            device_id=(s, dev_sib),
            device_id_type=MESH,
        ).wait_recv()

    def layer(k):
        c = lax.div(k, PASS)
        piece = lax.rem(k, PIECES)
        squares = jnp.zeros((PIECE, 128), jnp.float32)
        for j in range(CHUNKS):
            hop_arrived(k, j)
            wide = inbox[k, j].astype(jnp.float32)
            for p in range(CW // 128):
                part = wide[:, p * 128 : (p + 1) * 128]
                squares = squares + part * part
            scaled = (wide * gain_ref[c, :, j * CW : (j + 1) * CW]).astype(jnp.bfloat16)
            for n in (3, 0, 1, 2):
                cols = slice(n * 512, (n + 1) * 512)
                product = jnp.dot(
                    scaled,
                    wq[c, j * CW : (j + 1) * CW, cols],
                    preferred_element_type=jnp.float32,
                )
                if j > 0:
                    product = product + acc[:, cols]
                acc[:, cols] = product
        inv = lax.rsqrt(jnp.sum(squares, axis=1, keepdims=True) * (1.0 / D) + EPS)

        def projected(col, width=HEAD_DIM):
            cols = slice(col, col + width)
            return acc[:, cols] * inv + bias_ref[c, :, cols]

        def rotated(value, table):
            turned = pltpu.roll(value, HEAD_DIM // 2, 1)
            return value * rope_ref[piece, table] + turned * rope_ref[piece, table + 1]

        rows = pl.ds(pl.multiple_of(piece * PIECE, PIECE), PIECE)
        for g in range(KV_HEADS):
            key_high, key_low = split_two(rotated(projected(D + g * HEAD_DIM), 2))
            keys[g, rows, :HEAD_DIM] = key_high
            keys[g, rows, HEAD_DIM:] = key_low
            value_rows = projected(D + (KV_HEADS + g) * HEAD_DIM)
            values[g, rows, :HEAD_DIM] = value_rows.astype(jnp.bfloat16)
        contract = (((1,), (1,)), ((), ()))
        mask = jnp.concatenate([mask_ref[piece]] * GROUP, axis=0)
        scores = []
        for g in range(KV_HEADS):
            heads = [
                split_two(rotated(projected((g * GROUP + h) * HEAD_DIM), 0))
                for h in range(GROUP)
            ]
            query_high = jnp.concatenate([h[0] for h in heads], axis=0)
            query_low = jnp.concatenate([h[1] for h in heads], axis=0)
            key_high = keys[g, :, :HEAD_DIM]
            key_low = keys[g, :, HEAD_DIM:]
            scores.append(
                lax.dot_general(
                    jnp.concatenate([query_high, query_low, query_high], axis=1),
                    jnp.concatenate([key_high, key_high, key_low], axis=1),
                    contract,
                    preferred_element_type=jnp.float32,
                )
            )
        weights = []
        for g in range(KV_HEADS):
            masked = scores[g] + mask
            shifted = masked - jnp.max(masked, axis=1, keepdims=True)
            weights.append(jnp.exp(shifted).astype(jnp.bfloat16))
        mixed = [
            jnp.dot(weights[g], values[g], preferred_element_type=jnp.float32)
            for g in range(KV_HEADS)
        ]
        contexts = []
        for g in range(KV_HEADS):
            context = (mixed[g][:, :HEAD_DIM] / mixed[g][:, HEAD_DIM:]).astype(jnp.bfloat16)
            contexts.append(
                jnp.concatenate(
                    [context[h * PIECE : (h + 1) * PIECE] for h in range(GROUP)], axis=1
                )
            )

        updates = [None] * CHUNKS
        half = GROUP * HEAD_DIM

        def finish(j):
            total = inbox[k, j].astype(jnp.float32) + updates[j]
            outbox[k, j] = total.astype(jnp.bfloat16)
            hop(k, j).start()

        for j in range(CHUNKS):
            for g in range(KV_HEADS):
                product = jnp.dot(
                    contexts[g],
                    wo[c, g * half : (g + 1) * half, j * CW : (j + 1) * CW],
                    preferred_element_type=jnp.float32,
                )
                updates[j] = product if g == 0 else updates[j] + product
            if j > 0:
                finish(j - 1)
        finish(CHUNKS - 1)

    def step(k, carry):
        layer(k)

        @pl.when(k == 4)
        def _():
            gather_b(2)

        @pl.when(k == 7)
        def _():
            gather_b(3)
            gather_c(2)
            gather_c(3)

        @pl.when(k == 9)
        def _():
            gather_d(2)
            gather_d(3)

        @pl.when(k == 15)
        def _():
            for t in (2, 3):
                gather_e(t)
                gather_f(t)

        return carry

    lax.fori_loop(0, STEPS, step, 0)

    pltpu.make_async_remote_copy(
        src_ref=outbox,
        dst_ref=outbox,
        send_sem=hsend.at[0],
        recv_sem=hrecv.at[0, 0],
        device_id=(s, dev_sib),
        device_id_type=MESH,
    ).wait_send()
    for t in range(4):
        gather_sent(t)

    finished = inbox.at[pl.ds(FINAL, PIECES)]
    pltpu.make_async_remote_copy(
        src_ref=finished,
        dst_ref=finished,
        send_sem=hsend.at[0],
        recv_sem=hrecv.at[PASS, 0],
        device_id=(s, dev_sib),
        device_id_type=MESH,
    ).wait_recv()
    for n in range(PIECES):
        for j in range(CHUNKS):
            result_ref[n * PIECE : (n + 1) * PIECE, j * CW : (j + 1) * CW] = inbox[FINAL + n, j]


def per_device(hidden_in, norm_gain, qkv_weight, qkv_bias, out_weight):
    rope, mask = tables()
    vmem = pl.BlockSpec(memory_space=pltpu.VMEM)
    anywhere = pl.BlockSpec(memory_space=pl.ANY)
    dma = pltpu.SemaphoreType.DMA
    result = pl.pallas_call(
        kernel,
        name="sections",
        out_shape=jax.ShapeDtypeStruct((LEN, D), jnp.bfloat16),
        in_specs=[anywhere, vmem, anywhere, vmem, anywhere, vmem, vmem],
        out_specs=vmem,
        scratch_shapes=[
            pltpu.VMEM((2, D, QKV), jnp.bfloat16),
            pltpu.VMEM((2, D, D), jnp.bfloat16),
            pltpu.VMEM((STEPS + PIECES, CHUNKS, PIECE, CW), jnp.bfloat16),
            pltpu.VMEM((STEPS, CHUNKS, PIECE, CW), jnp.bfloat16),
            pltpu.VMEM((PIECE, QKV), jnp.float32),
            pltpu.VMEM((KV_HEADS, LEN, 2 * HEAD_DIM), jnp.bfloat16),
            pltpu.VMEM((KV_HEADS, LEN, 2 * HEAD_DIM), jnp.bfloat16),
            dma((4,)),
            dma((4,)),
            dma((4, 8)),
            dma((1,)),
            dma((PASS + 1, CHUNKS)),
        ],
        compiler_params=pltpu.CompilerParams(collective_id=0, has_side_effects=True),
    )(hidden_in, norm_gain, qkv_weight, qkv_bias, out_weight, rope, mask)
    return result[None, None]


def solution(mesh):
    in_specs = (
        P(None, "fsdp", None, None),
        P(None, "section", None),
        P(None, "section", "fsdp", None),
        P(None, "section", None),
        P(None, "section", "fsdp", None),
    )
    out_specs = P("section", "fsdp", None, None)
    return jax.shard_map(
        per_device, mesh=mesh, in_specs=in_specs, out_specs=out_specs, check_vma=False
    )
```
